32 devices in a mesh: rep: 2 (over x), amp: 16 (over z, y, core).
Axes of the slice: x: 2, y: 2, z: 4, core: 2. Of those that a mesh axis runs over, the one named last changes fastest.
Arguments:
- amplitudes: float32 [2, 1048576], P(None, ('rep', 'amp')), parts along dimension 1, may hold values from -12 to 12
- coupling_index: int32 [4, 18], P('rep'), parts along dimension 0, may hold values from 0 to 15
- rotation_index: int32 [4, 19], P('rep'), parts along dimension 0, may hold values from 0 to 15
- chain_order: int32 [19], replicated, may hold values from 0 to 18, each once
- bond_sign: int32 [18], replicated, may hold values 0 or 1
Outputs:
- final_state: float32 [2, 1048576], P(None, ('rep', 'amp')), parts along dimension 1
- energies: float32 [4], P('rep'), parts along dimension 0
The draws below stay inside these ranges and needn't reach their ends.
There are 2 independent parts, one for each index of `rep`. The reference program is written for one: setup_inputs(seed, part) draws one part's arguments, and reference() takes and returns one part's arrays. A program takes and returns all parts, laid end to end along the dimension named above; an argument that names none is the same for every part. Nothing has to cross between parts.
Inputs may be any that keep to these rules, and one draw needn't show every extreme that they name: chain_order holds each of 0 to 18 once.
All inputs are finite; a program needn't handle non-finite values.
Results may differ from the reference program's by a relative error of at most 0.0003.
Values sent between devices are 32-bit elements; how exact they have to be, the bound alone decides.
A program may use at most 128 MiB of HBM per device.

```python
import jax
import jax.numpy as jnp
from jax import lax

LQ = 15
NQ = 19
AMPS = 524288
LAYERS = 2
ANGLES = 16


def draw_amplitudes(key, part):
    devices_count = AMPS // 2 ** LQ
    owner = jnp.arange(AMPS, dtype=jnp.int32) // 2 ** LQ
    ramp = owner.astype(jnp.float32) / jnp.float32(max(devices_count - 1, 1))
    values = jnp.clip(jax.random.normal(key, (2, AMPS), jnp.float32), -4.0, 4.0)
    scaling = 1.0 + 2.0 * ramp
    return (values * scaling[None, :]).astype(jnp.float32)


def with_ends(entries, own_key, least, largest):
    extent = entries.shape
    place = [jax.random.randint(jax.random.fold_in(own_key, axis), (), 0, extent[axis]) for axis in range(len(extent))]
    entries = entries.at[tuple(place)].set(least)
    longest = extent.index(max(extent))
    place[longest] = (place[longest] + 1) % extent[longest]
    return entries.at[tuple(place)].set(largest)


def setup_inputs(seed: int = 0, part: int = 0) -> dict:
    key_list = jax.random.split(jax.random.key(seed), 6)
    part_splits = jax.random.split(jax.random.fold_in(key_list[5], part), 6)
    return {
        "amplitudes": draw_amplitudes(jax.random.fold_in(jax.random.fold_in(key_list[5], part), 71), part),
        "coupling_index": with_ends(jax.random.randint(part_splits[1], (LAYERS, NQ - 1), 0, ANGLES), jax.random.fold_in(part_splits[1], 1), 0, ANGLES - 1).astype(jnp.int32),
        "rotation_index": with_ends(jax.random.randint(part_splits[2], (LAYERS, NQ), 0, ANGLES), jax.random.fold_in(part_splits[2], 1), 0, ANGLES - 1).astype(jnp.int32),
        "chain_order": jax.random.permutation(key_list[3], NQ).astype(jnp.int32),
        "bond_sign": with_ends((jax.random.randint(key_list[4], (NQ - 1,), 0, 4) < 3).astype(jnp.int32), jax.random.fold_in(key_list[4], 1), 0, 1),
    }


def angle_table():
    return (jnp.arange(ANGLES, dtype=jnp.float32) + 1.0) * (jnp.float32(jnp.pi) / (2.0 * (ANGLES + 1)))

def lookup(index):
    hits = index[..., None] == jnp.arange(ANGLES, dtype=jnp.int32)
    return lax.optimization_barrier(jnp.sum(jnp.where(hits, angle_table(), jnp.float32(0.0)), axis=-1))

def reference(amplitudes, coupling_index, rotation_index, chain_order, bond_sign):
    bond_signs = (2 * bond_sign - 1).astype(jnp.float32)
    couple_angles = lookup(coupling_index) * bond_signs[None, :]
    turn_angles = lookup(rotation_index)
    positions = jnp.arange(AMPS, dtype=jnp.int32)
    energy_field = jnp.zeros((AMPS,), jnp.float32)
    phase_fields = [jnp.zeros((AMPS,), jnp.float32) for layer_index in range(LAYERS)]
    for bond_index in range(NQ - 1):
        differ = jnp.right_shift(positions, chain_order[bond_index]) ^ jnp.right_shift(positions, chain_order[bond_index + 1])
        parity_sign = (1 - 2 * (differ & 1)).astype(jnp.float32)
        energy_field = energy_field + bond_signs[bond_index] * parity_sign
        for layer_index in range(LAYERS):
            phase_fields[layer_index] = phase_fields[layer_index] + couple_angles[layer_index, bond_index] * parity_sign
    total_norm = jnp.sum(amplitudes * amplitudes)
    factor = 1.0 / jnp.sqrt(total_norm / AMPS + 1e-06)
    real_part = amplitudes[0] * factor
    imag_part = amplitudes[1] * factor
    energies = []
    for layer_index in range(LAYERS):
        cosine = jnp.cos(phase_fields[layer_index])
        sine_part = jnp.sin(phase_fields[layer_index])
        real_part, imag_part = (cosine * real_part + sine_part * imag_part, cosine * imag_part - sine_part * real_part)
        for qubit in range(NQ):
            cosine = jnp.cos(turn_angles[layer_index, qubit])
            sine_part = jnp.sin(turn_angles[layer_index, qubit])
            shape = (AMPS // 2 ** (qubit + 1), 2, 2 ** qubit)
            real_view = real_part.reshape(shape)
            imag_view = imag_part.reshape(shape)
            real_low, real_high = (real_view[:, 0], real_view[:, 1])
            imag_low, imag_high = (imag_view[:, 0], imag_view[:, 1])
            new_real = jnp.stack([cosine * real_low + sine_part * imag_high, cosine * real_high + sine_part * imag_low], axis=1)
            new_imag = jnp.stack([cosine * imag_low - sine_part * real_high, cosine * imag_high - sine_part * real_low], axis=1)
            real_part = new_real.reshape(AMPS)
            imag_part = new_imag.reshape(AMPS)
        weight = real_part * real_part + imag_part * imag_part
        energies.append(jnp.sum(weight * energy_field) / AMPS)
    return (jnp.stack([real_part, imag_part]), jnp.stack(energies))
```

```python
import functools
import math

import jax
import jax.numpy as jnp
from jax import lax
from jax.experimental import pallas as pl
from jax.experimental.pallas import tpu as pltpu
from jax.sharding import PartitionSpec as P

LAYERS = 2
ANGLES = 16
LANES = 128
LANE_BITS = 7
F32 = jnp.float32
BF16 = jnp.bfloat16
MESH = pl.DeviceIdType.MESH


def angle(index):
    return (index + 1).astype(F32) * F32(math.pi / (2.0 * (ANGLES + 1)))


def mm(left, right):
    return jnp.dot(left, right, preferred_element_type=F32)


def split(values):
    high = values.astype(BF16)
    return high, (values - high.astype(F32)).astype(BF16)


def mm3(left, right):
    return mm(left[0], right[0]) + mm(left[1], right[0]) + mm(left[0], right[1])


def mm_exact_left(left, values):
    high = values.astype(BF16)
    rest = values - high.astype(F32)
    middle = rest.astype(BF16)
    low = (rest - middle.astype(F32)).astype(BF16)
    return mm(left, high) + mm(left, middle) + mm(left, low)


def mm_exact_right(values, right):
    high = values.astype(BF16)
    rest = values - high.astype(F32)
    middle = rest.astype(BF16)
    low = (rest - middle.astype(F32)).astype(BF16)
    return mm(high, right) + mm(middle, right) + mm(low, right)


def sin_cos(values):
    turns = jnp.floor(values * F32(1.0 / math.pi) + 0.5)
    rest = values - turns * F32(3.140625)
    rest = rest - turns * F32(9.67502593994140625e-4)
    rest = rest - turns * F32(1.509957990978376432e-7)
    sign = 1.0 - 2.0 * (turns - 2.0 * jnp.floor(turns * 0.5))
    square = rest * rest
    sine = F32(-1.0 / 39916800)
    for coefficient in (1.0 / 362880, -1.0 / 5040, 1.0 / 120, -1.0 / 6, 1.0):
        sine = sine * square + F32(coefficient)
    cosine = F32(-1.0 / 3628800)
    for coefficient in (1.0 / 40320, -1.0 / 720, 1.0 / 24, -0.5, 1.0):
        cosine = cosine * square + F32(coefficient)
    return sine * (rest * sign), cosine * sign


def gate_matrix(pairs):
    base = min(len(pairs), LANE_BITS)
    size = 2**base
    differ = lax.broadcasted_iota(jnp.int32, (size, size), 0) ^ lax.broadcasted_iota(
        jnp.int32, (size, size), 1
    )
    count = jnp.zeros((size, size), jnp.int32)
    value = jnp.ones((size, size), F32)
    for bit, (cosine, sine) in enumerate(pairs[:base]):
        flag = (differ >> bit) & 1
        count = count + flag
        value = value * jnp.where(flag == 1, sine, cosine)
    value = jnp.where(((count + 1) & 2) == 2, -value, value)
    odd = (count & 1) == 1
    real, imag = jnp.where(odd, 0.0, value), jnp.where(odd, value, 0.0)
    for cosine, sine in pairs[base:]:
        same_real, same_imag = cosine * real, cosine * imag
        flip_real, flip_imag = sine * imag, -sine * real

        def block(same, flip):
            return jnp.concatenate(
                [
                    jnp.concatenate([same, flip], axis=1),
                    jnp.concatenate([flip, same], axis=1),
                ],
                axis=0,
            )

        real, imag = block(same_real, flip_real), block(same_imag, flip_imag)
    return real, imag


def lane_operand(pairs):
    real, imag = gate_matrix(pairs)
    return split(
        jnp.concatenate(
            [jnp.concatenate([real, imag], axis=1), jnp.concatenate([-imag, real], axis=1)],
            axis=0,
        )
    )


def row_operand(pairs):
    return split(jnp.concatenate(gate_matrix(pairs), axis=0))


def apply_lanes(real, imag, operand):
    both = mm3(split(jnp.concatenate([real, imag], axis=1)), operand)
    return both[:, :LANES], both[:, LANES:]


def apply_rows(real, imag, operand):
    rows = real.shape[0]
    both = mm3(operand, split(jnp.concatenate([real, imag], axis=1)))
    return (
        both[:rows, :LANES] - both[rows:, LANES:],
        both[:rows, LANES:] + both[rows:, :LANES],
    )


def apply_top(real, imag, pairs, block_rows):
    rows = real.shape[0]
    if block_rows % 8:
        low = block_rows.bit_length() - 1
        pairs = [(F32(1.0), F32(0.0))] * low + pairs
        return apply_rows(real, imag, row_operand(pairs))
    for bit, (cosine, sine) in enumerate(pairs):
        width = block_rows << bit
        real_parts, imag_parts = [], []
        for start in range(0, rows, 2 * width):
            low, high = slice(start, start + width), slice(start + width, start + 2 * width)
            real_parts += [
                cosine * real[low] + sine * imag[high],
                cosine * real[high] + sine * imag[low],
            ]
            imag_parts += [
                cosine * imag[low] - sine * real[high],
                cosine * imag[high] - sine * real[low],
            ]
        real = jnp.concatenate(real_parts, axis=0)
        imag = jnp.concatenate(imag_parts, axis=0)
    return real, imag


def kernel(
    axis, count, chunks, qubits,
    state_hbm, couple_hbm, turn_hbm, order_hbm, sign_hbm,
    out_ref, energy_ref,
    state_ref, couple_ref, turn_ref, order_ref, sign_ref,
    table, send, recv, stat_send, stat_recv, plane_real, plane_imag,
    local_sems, send_sems, recv_sems, stat_send_sems, stat_recv_sems,
):
    me = lax.axis_index(axis)
    rows = state_ref.shape[0] // 2
    row_bits = rows.bit_length() - 1
    global_bits = count.bit_length() - 1
    local_bits = row_bits + LANE_BITS
    block_rows = rows // count
    low_bits = row_bits - global_bits
    chunk_bits = chunks.bit_length() - 1
    chunk_rows = block_rows // chunks
    inner_bits = low_bits - chunk_bits
    part_rows = rows // chunks
    order = sorted(range(1, count), key=lambda step: abs(count // 2 - step))
    peers = {step: lax.rem(me + step, count) for step in order}

    barrier = pltpu.get_barrier_semaphore()
    arrivals = [
        pltpu.make_async_copy(source, target, local_sems.at[number])
        for number, (source, target) in enumerate(
            [
                (couple_hbm, couple_ref),
                (turn_hbm, turn_ref),
                (order_hbm, order_ref),
                (sign_hbm, sign_ref),
                (state_hbm, state_ref),
            ]
        )
    ]
    for copy in arrivals:
        copy.start()

    for step in order:
        pl.semaphore_signal(barrier, inc=1, device_id={axis: peers[step]}, device_id_type=MESH)

    for entry in range(ANGLES):
        theta = (entry + 1) * math.pi / (2.0 * (ANGLES + 1))
        table[0, entry] = F32(math.cos(theta))
        table[1, entry] = F32(math.sin(theta))
    for copy in arrivals[:-1]:
        copy.wait()

    def turn(layer, qubit):
        index = turn_ref[layer, qubit]
        return table[0, index], table[1, index]

    height = -(-qubits // 8) * 8
    place = lax.broadcasted_iota(jnp.int32, (height, LANES), 0) * LANES + (
        lax.broadcasted_iota(jnp.int32, (height, LANES), 1)
    )

    def couplings(layers):
        matrices = [jnp.zeros((height, LANES), F32) for _ in layers]
        for bond in range(qubits - 1):
            start, end = order_ref[bond], order_ref[bond + 1]
            here = (place == start * LANES + end) | (place == end * LANES + start)
            for number, layer in enumerate(layers):
                value = (2 * sign_ref[bond] - 1).astype(F32)
                if layer < LAYERS:
                    value = angle(couple_ref[layer, bond]) * value
                matrices[number] = jnp.where(here, value, matrices[number])
        rest = jnp.zeros((LANES - height, LANES), F32)
        return [jnp.concatenate([matrix, rest], axis=0) for matrix in matrices]

    square_row = lax.broadcasted_iota(jnp.int32, (LANES, LANES), 0)
    square_lane = lax.broadcasted_iota(jnp.int32, (LANES, LANES), 1)
    lane_spin = (1 - 2 * ((square_lane >> jnp.minimum(square_row, 31)) & 1)).astype(F32)
    lane_only = jnp.where(square_row < LANE_BITS, lane_spin, 0.0)
    lane_ones = jnp.where(square_row < LANE_BITS, lane_spin, 1.0).astype(BF16)
    row_index = lax.broadcasted_iota(jnp.int32, (rows, LANES), 0)
    lane_index = lax.broadcasted_iota(jnp.int32, (rows, LANES), 1)

    def row_spin(swapped, chunked):
        held = row_index
        if chunked:
            inner = held & (chunk_rows - 1)
            block = (held >> inner_bits) & (count - 1)
            chunk = held >> (inner_bits + global_bits)
            held = inner + (chunk << inner_bits) + (block << low_bits)
        if swapped:
            low, high = held & (block_rows - 1), held >> low_bits
            index = low + (me << low_bits) + (high << row_bits)
        else:
            index = held + (me << row_bits)
        spin = (1 - 2 * ((index >> jnp.clip(lane_index - LANE_BITS, 0, 31)) & 1)).astype(F32)
        return jnp.where((lane_index >= LANE_BITS) & (lane_index < qubits), spin, 0.0)

    def field(spin, matrix, exact):
        if exact:
            half = mm(spin.astype(BF16), matrix.astype(BF16))
        else:
            half = mm_exact_left(spin.astype(BF16), matrix)
        half = jnp.where(lane_index < LANE_BITS, half, 0.5 * half * spin)
        lane_pairs = 0.5 * jnp.sum(
            mm_exact_right(matrix, lane_only.astype(BF16)) * lane_only, axis=0, keepdims=True
        )
        if exact:
            return mm(half.astype(BF16), lane_ones) + lane_pairs
        return mm_exact_right(half, lane_ones) + lane_pairs

    def copies(layer, chunk):
        return [
            pltpu.make_async_remote_copy(
                src_ref=send.at[layer, chunk, peers[step]],
                dst_ref=recv.at[layer, chunk, me],
                send_sem=send_sems.at[layer, chunk],
                recv_sem=recv_sems.at[layer, chunk],
                device_id={axis: peers[step]},
                device_id_type=MESH,
            )
            for step in order
        ]

    def stat_copies(which):
        return [
            pltpu.make_async_remote_copy(
                src_ref=stat_send.at[which],
                dst_ref=stat_recv.at[which, me],
                send_sem=stat_send_sems.at[which],
                recv_sem=stat_recv_sems.at[which],
                device_id={axis: peers[step]},
                device_id_type=MESH,
            )
            for step in order
        ]

    others = pl.ds(0, count - 1)

    def blocks(layer, chunk):
        return pltpu.make_async_remote_copy(
            src_ref=send.at[layer, chunk, others],
            dst_ref=recv.at[layer, chunk, others],
            send_sem=send_sems.at[layer, chunk],
            recv_sem=recv_sems.at[layer, chunk],
            device_id={axis: peers[order[0]]},
            device_id_type=MESH,
        )

    def stats(which):
        return pltpu.make_async_remote_copy(
            src_ref=stat_recv.at[which, others],
            dst_ref=stat_recv.at[which, others],
            send_sem=stat_send_sems.at[which],
            recv_sem=stat_recv_sems.at[which],
            device_id={axis: peers[order[0]]},
            device_id_type=MESH,
        )

    def pack(layer, chunk, real, imag, first_row, stride):
        for block in range(count):
            start = first_row + block * stride
            part = slice(start, start + chunk_rows)
            send[layer, chunk, block, :chunk_rows, :] = real[part]
            send[layer, chunk, block, chunk_rows:, :] = imag[part]

    def received(layer, chunk):
        if chunk_rows % 8 == 0:
            return (
                jnp.concatenate([recv[layer, chunk, b, :chunk_rows, :] for b in range(count)], axis=0),
                jnp.concatenate([recv[layer, chunk, b, chunk_rows:, :] for b in range(count)], axis=0),
            )
        for block in range(count):
            part = slice(block * chunk_rows, (block + 1) * chunk_rows)
            plane_real[part, :] = recv[layer, chunk, block, :chunk_rows, :]
            plane_imag[part, :] = recv[layer, chunk, block, chunk_rows:, :]
        return plane_real[...], plane_imag[...]

    def part_of(values, chunk):
        return values[chunk * part_rows : (chunk + 1) * part_rows]

    def turned(real, imag, pairs):
        return apply_top(real, imag, pairs, chunk_rows)

    sine, cosine = sin_cos(field(row_spin(False, False), couplings([0])[0], False))
    lanes = lane_operand([turn(0, qubit) for qubit in range(LANE_BITS)])
    held = row_operand([turn(0, LANE_BITS + bit) for bit in range(row_bits)])

    arrivals[-1].wait()
    real = state_ref[pl.ds(0, rows, 2), :]
    imag = state_ref[pl.ds(1, rows, 2), :]
    stat_send[0] = jnp.sum(real * real + imag * imag, axis=0, keepdims=True)
    real, imag = cosine * real + sine * imag, cosine * imag - sine * real
    real, imag = apply_lanes(real, imag, lanes)
    real, imag = apply_rows(real, imag, held)
    first = [copies(0, chunk) for chunk in range(chunks)]
    second = [copies(1, chunk) for chunk in range(chunks)]
    norms, weights = stat_copies(0), stat_copies(1)
    for chunk in range(chunks):
        pack(0, chunk, real, imag, chunk * chunk_rows, block_rows)
    pl.semaphore_wait(barrier, count - 1)
    for copy in first[0]:
        copy.start()
    for chunk in range(chunks):
        recv[0, chunk, me] = send[0, chunk, me]
    stat_recv[0, me] = stat_send[0]

    moved = row_spin(True, True)
    next_bonds, sign_bonds = couplings([1, LAYERS])
    sine, cosine = sin_cos(field(moved, next_bonds, False))
    for later in first[1:] + [norms]:
        for copy in later:
            copy.start()
    lanes = lane_operand([turn(1, qubit) for qubit in range(LANE_BITS)])
    held = row_operand(
        [turn(1, LANE_BITS + bit) for bit in range(inner_bits)]
        + [turn(1, local_bits + bit) for bit in range(global_bits)]
    )
    late = [turn(1, LANE_BITS + inner_bits + bit) for bit in range(chunk_bits)]
    tops = [
        [turn(0, local_bits + bit) for bit in range(global_bits)],
        [turn(1, local_bits - global_bits + bit) for bit in range(global_bits)],
    ]
    energy_moved = field(moved, sign_bonds, True)
    energy_plain = field(row_spin(False, True), sign_bonds, True)

    between = []
    for chunk in range(chunks):
        blocks(0, chunk).wait_recv()
        real, imag = received(0, chunk)
        real, imag = turned(real, imag, tops[0])
        between.append((real, imag))
        part_sine, part_cosine = part_of(sine, chunk), part_of(cosine, chunk)
        real, imag = (
            part_cosine * real + part_sine * imag,
            part_cosine * imag - part_sine * real,
        )
        real, imag = apply_lanes(real, imag, lanes)
        real, imag = apply_rows(real, imag, held)
        pack(1, chunk, real, imag, 0, chunk_rows)
        for copy in second[chunk]:
            copy.start()
        recv[1, chunk, me] = send[1, chunk, me]

    def folded(parts, energy_field):
        total = jnp.zeros((1, LANES), F32)
        for chunk, (real, imag) in enumerate(parts):
            weight = (real * real + imag * imag) * part_of(energy_field, chunk)
            total = total + jnp.sum(weight, axis=0, keepdims=True)
        return total + pltpu.roll(total, LANES // 2, 1)

    energy_first = folded(between, energy_moved)
    stats(0).wait_recv()
    amps_total = F32(2.0**qubits)
    norm = jnp.sum(jnp.sum(stat_recv[0], axis=0), axis=1, keepdims=True)
    factor = 1.0 / jnp.sqrt(norm / amps_total + 1e-06)

    parts = []
    for chunk in range(chunks):
        blocks(1, chunk).wait_recv()
        real, imag = received(1, chunk)
        parts.append(turned(real, imag, tops[1]))
    for bit, (cosine, sine) in enumerate(late):
        fresh = list(parts)
        for low in range(chunks):
            high = low | 1 << bit
            if high == low:
                continue
            (low_real, low_imag), (high_real, high_imag) = parts[low], parts[high]
            fresh[low] = (cosine * low_real + sine * high_imag, cosine * low_imag - sine * high_real)
            fresh[high] = (cosine * high_real + sine * low_imag, cosine * high_imag - sine * low_real)
        parts = fresh

    lane = lax.broadcasted_iota(jnp.int32, (1, LANES), 1)
    stat_send[1] = jnp.where(lane < LANES // 2, energy_first, folded(parts, energy_plain))
    for copy in weights:
        copy.start()
    stat_recv[1, me] = stat_send[1]
    for chunk, (real, imag) in enumerate(parts):
        real, imag = real * factor, imag * factor
        for block in range(count):
            start = 2 * (block * block_rows + chunk * chunk_rows)
            part = slice(block * chunk_rows, (block + 1) * chunk_rows)
            out_ref[pl.ds(start, chunk_rows, 2), :] = real[part]
            out_ref[pl.ds(start + 1, chunk_rows, 2), :] = imag[part]
    for layer in range(LAYERS):
        for chunk in range(chunks):
            blocks(layer, chunk).wait_send()
    stats(0).wait_send()
    stats(1).wait_recv()
    sums = jnp.sum(stat_recv[1], axis=0) * (factor * factor / amps_total)
    low_sum = jnp.sum(jnp.where(lane < LANES // 2, sums, 0.0), axis=1, keepdims=True)
    high_sum = jnp.sum(jnp.where(lane < LANES // 2, 0.0, sums), axis=1, keepdims=True)
    which = lax.broadcasted_iota(jnp.int32, (1, LAYERS), 1)
    energy_ref[...] = jnp.where(which == 0, low_sum, high_sum)
    stats(1).wait_send()


def solution(mesh):
    axis = "amp"
    count = mesh.shape[axis]

    def local(amplitudes, coupling_index, rotation_index, chain_order, bond_sign):
        rows = amplitudes.shape[1] // LANES
        qubits = chain_order.shape[0]
        block_rows = rows // count
        chunks = 2 if block_rows % 16 == 0 else 1
        chunk_rows = block_rows // chunks
        view = amplitudes.reshape(2, rows, LANES).transpose(1, 0, 2).reshape(2 * rows, LANES)
        vmem = pl.BlockSpec(memory_space=pltpu.VMEM)
        anywhere = pl.BlockSpec(memory_space=pl.ANY)
        state, energies = pl.pallas_call(
            functools.partial(kernel, axis, count, chunks, qubits),
            out_shape=(
                pltpu.VMEM((2 * rows, LANES), F32),
                pltpu.VMEM((1, LAYERS), F32),
            ),
            in_specs=[anywhere] * 5,
            out_specs=(vmem, vmem),
            scratch_shapes=[
                pltpu.VMEM((2 * rows, LANES), F32),
                pltpu.SMEM(coupling_index.shape, jnp.int32),
                pltpu.SMEM(rotation_index.shape, jnp.int32),
                pltpu.SMEM(chain_order.shape, jnp.int32),
                pltpu.SMEM(bond_sign.shape, jnp.int32),
                pltpu.SMEM((2, ANGLES), F32),
                pltpu.VMEM((LAYERS, chunks, count, 2 * chunk_rows, LANES), F32),
                pltpu.VMEM((LAYERS, chunks, count, 2 * chunk_rows, LANES), F32),
                pltpu.VMEM((2, 1, LANES), F32),
                pltpu.VMEM((2, count, 1, LANES), F32),
                pltpu.VMEM((rows, LANES), F32),
                pltpu.VMEM((rows, LANES), F32),
                pltpu.SemaphoreType.DMA((5,)),
                pltpu.SemaphoreType.DMA((LAYERS, chunks)),
                pltpu.SemaphoreType.DMA((LAYERS, chunks)),
                pltpu.SemaphoreType.DMA((2,)),
                pltpu.SemaphoreType.DMA((2,)),
            ],
            compiler_params=pltpu.CompilerParams(collective_id=0, has_side_effects=True),
        )(view, coupling_index, rotation_index, chain_order, bond_sign)
        state = state.reshape(rows, 2, LANES).transpose(1, 0, 2).reshape(2, rows * LANES)
        return state, energies.reshape(LAYERS)

    in_specs = (P(None, ("rep", "amp")), P("rep", None), P("rep", None), P(), P())
    out_specs = (P(None, ("rep", "amp")), P("rep"))
    return jax.shard_map(local, mesh=mesh, in_specs=in_specs, out_specs=out_specs, check_vma=False)
```

```python
import functools
import math

import jax
import jax.numpy as jnp
from jax import lax
from jax.experimental import pallas as pl
from jax.experimental.pallas import tpu as pltpu
from jax.sharding import PartitionSpec as P

LAYERS = 2
ANGLES = 16
LANES = 128
LANE_BITS = 7
F32 = jnp.float32
BF16 = jnp.bfloat16
MESH = pl.DeviceIdType.MESH
DOWN = (3, 2, 1, 0)
PLANS = (
    (((2, 3, 1, 0), (2, 0, 3, 1)), ((1, 0, 2, 3), DOWN)),
    (((2, 3, 1, 0), DOWN), ((2, 3, 0, 1), DOWN)),
)


def angle(index):
    return (index + 1).astype(F32) * F32(math.pi / (2.0 * (ANGLES + 1)))


def mm(left, right):
    return jnp.dot(left, right, preferred_element_type=F32)


def split(values):
    high = values.astype(BF16)
    return high, (values - high.astype(F32)).astype(BF16)


def mm3(left, right):
    return mm(left[0], right[0]) + mm(left[1], right[0]) + mm(left[0], right[1])


def mm_exact_left(left, values):
    high = values.astype(BF16)
    rest = values - high.astype(F32)
    middle = rest.astype(BF16)
    low = (rest - middle.astype(F32)).astype(BF16)
    return mm(left, high) + mm(left, middle) + mm(left, low)


def mm_exact_right(values, right):
    high = values.astype(BF16)
    rest = values - high.astype(F32)
    middle = rest.astype(BF16)
    low = (rest - middle.astype(F32)).astype(BF16)
    return mm(high, right) + mm(middle, right) + mm(low, right)


def sin_cos(values):
    turns = jnp.floor(values * F32(1.0 / math.pi) + 0.5)
    rest = values - turns * F32(3.140625)
    rest = rest - turns * F32(9.67502593994140625e-4)
    rest = rest - turns * F32(1.509957990978376432e-7)
    sign = 1.0 - 2.0 * (turns - 2.0 * jnp.floor(turns * 0.5))
    square = rest * rest
    sine = F32(-1.0 / 39916800)
    for coefficient in (1.0 / 362880, -1.0 / 5040, 1.0 / 120, -1.0 / 6, 1.0):
        sine = sine * square + F32(coefficient)
    cosine = F32(-1.0 / 3628800)
    for coefficient in (1.0 / 40320, -1.0 / 720, 1.0 / 24, -0.5, 1.0):
        cosine = cosine * square + F32(coefficient)
    return sine * (rest * sign), cosine * sign


def gate_matrix(pairs):
    base = min(len(pairs), LANE_BITS)
    size = 2**base
    differ = lax.broadcasted_iota(jnp.int32, (size, size), 0) ^ lax.broadcasted_iota(
        jnp.int32, (size, size), 1
    )
    count = jnp.zeros((size, size), jnp.int32)
    value = jnp.ones((size, size), F32)
    for bit, (cosine, sine) in enumerate(pairs[:base]):
        flag = (differ >> bit) & 1
        count = count + flag
        value = value * jnp.where(flag == 1, sine, cosine)
    value = jnp.where(((count + 1) & 2) == 2, -value, value)
    odd = (count & 1) == 1
    real, imag = jnp.where(odd, 0.0, value), jnp.where(odd, value, 0.0)
    for cosine, sine in pairs[base:]:
        same_real, same_imag = cosine * real, cosine * imag
        flip_real, flip_imag = sine * imag, -sine * real

        def block(same, flip):
            return jnp.concatenate(
                [
                    jnp.concatenate([same, flip], axis=1),
                    jnp.concatenate([flip, same], axis=1),
                ],
                axis=0,
            )

        real, imag = block(same_real, flip_real), block(same_imag, flip_imag)
    return real, imag


def lane_operand(pairs):
    real, imag = gate_matrix(pairs)
    return split(
        jnp.concatenate(
            [jnp.concatenate([real, imag], axis=1), jnp.concatenate([-imag, real], axis=1)],
            axis=0,
        )
    )


def row_operand(pairs):
    return split(jnp.concatenate(gate_matrix(pairs), axis=0))


def apply_lanes(real, imag, operand):
    both = mm3(split(jnp.concatenate([real, imag], axis=1)), operand)
    return both[:, :LANES], both[:, LANES:]


def apply_rows(real, imag, operand):
    rows = real.shape[0]
    both = mm3(operand, split(jnp.concatenate([real, imag], axis=1)))
    return (
        both[:rows, :LANES] - both[rows:, LANES:],
        both[:rows, LANES:] + both[rows:, :LANES],
    )


def apply_top(real, imag, pairs, block_rows):
    rows = real.shape[0]
    if block_rows % 8:
        low = block_rows.bit_length() - 1
        pairs = [(F32(1.0), F32(0.0))] * low + pairs
        return apply_rows(real, imag, row_operand(pairs))
    for bit, (cosine, sine) in enumerate(pairs):
        width = block_rows << bit
        real_parts, imag_parts = [], []
        for start in range(0, rows, 2 * width):
            low, high = slice(start, start + width), slice(start + width, start + 2 * width)
            real_parts += [
                cosine * real[low] + sine * imag[high],
                cosine * real[high] + sine * imag[low],
            ]
            imag_parts += [
                cosine * imag[low] - sine * real[high],
                cosine * imag[high] - sine * real[low],
            ]
        real = jnp.concatenate(real_parts, axis=0)
        imag = jnp.concatenate(imag_parts, axis=0)
    return real, imag


def kernel(
    axis, count, chunks, qubits,
    state_hbm, couple_hbm, turn_hbm, order_hbm, sign_hbm,
    out_ref, energy_ref,
    state_ref, couple_ref, turn_ref, order_ref, sign_ref,
    table, send, recv, stat_send, stat_recv, plane_real, plane_imag,
    local_sems, send_sems, recv_sems, stat_send_sems, stat_recv_sems,
):
    me = lax.axis_index(axis)
    rows = state_ref.shape[0] // 2
    row_bits = rows.bit_length() - 1
    global_bits = count.bit_length() - 1
    local_bits = row_bits + LANE_BITS
    block_rows = rows // count
    low_bits = row_bits - global_bits
    chunk_bits = chunks.bit_length() - 1
    chunk_rows = block_rows // chunks
    inner_bits = low_bits - chunk_bits
    part_rows = rows // chunks
    def ranked(groups, inner):
        size = count // 4
        steps = [
            group * size + high * (size // 4) + low
            for group in groups
            for high in inner
            for low in range(size // 4)
        ]
        return [step for step in steps if step]

    order = ranked((2, 3, 1, 0), (3, 2, 1, 0))
    plans = [[ranked(*plan) for plan in layer] for layer in PLANS]
    flips = [(1 - 2 * lax.rem(me // 2**bit, 2)) * 2**bit for bit in range(global_bits)]
    peers = {
        step: me + sum(flips[bit] for bit in range(global_bits) if step >> bit & 1)
        for step in order
    }

    barrier = pltpu.get_barrier_semaphore()
    arrivals = [
        pltpu.make_async_copy(source, target, local_sems.at[number])
        for number, (source, target) in enumerate(
            [
                (couple_hbm, couple_ref),
                (turn_hbm, turn_ref),
                (order_hbm, order_ref),
                (sign_hbm, sign_ref),
                (state_hbm, state_ref),
            ]
        )
    ]
    for copy in arrivals:
        copy.start()

    for step in order:
        pl.semaphore_signal(barrier, inc=1, device_id={axis: peers[step]}, device_id_type=MESH)

    for entry in range(ANGLES):
        theta = (entry + 1) * math.pi / (2.0 * (ANGLES + 1))
        table[0, entry] = F32(math.cos(theta))
        table[1, entry] = F32(math.sin(theta))
    for copy in arrivals[:-1]:
        copy.wait()

    def turn(layer, qubit):
        index = turn_ref[layer, qubit]
        return table[0, index], table[1, index]

    height = -(-qubits // 8) * 8
    place = lax.broadcasted_iota(jnp.int32, (height, LANES), 0) * LANES + (
        lax.broadcasted_iota(jnp.int32, (height, LANES), 1)
    )

    def couplings(layers):
        matrices = [jnp.zeros((height, LANES), F32) for _ in layers]
        for bond in range(qubits - 1):
            start, end = order_ref[bond], order_ref[bond + 1]
            here = (place == start * LANES + end) | (place == end * LANES + start)
            for number, layer in enumerate(layers):
                value = (2 * sign_ref[bond] - 1).astype(F32)
                if layer < LAYERS:
                    value = angle(couple_ref[layer, bond]) * value
                matrices[number] = jnp.where(here, value, matrices[number])
        rest = jnp.zeros((LANES - height, LANES), F32)
        return [jnp.concatenate([matrix, rest], axis=0) for matrix in matrices]

    square_row = lax.broadcasted_iota(jnp.int32, (LANES, LANES), 0)
    square_lane = lax.broadcasted_iota(jnp.int32, (LANES, LANES), 1)
    lane_spin = (1 - 2 * ((square_lane >> jnp.minimum(square_row, 31)) & 1)).astype(F32)
    lane_only = jnp.where(square_row < LANE_BITS, lane_spin, 0.0)
    lane_ones = jnp.where(square_row < LANE_BITS, lane_spin, 1.0).astype(BF16)
    row_index = lax.broadcasted_iota(jnp.int32, (rows, LANES), 0)
    lane_index = lax.broadcasted_iota(jnp.int32, (rows, LANES), 1)

    def row_spin(swapped, chunked):
        held = row_index
        if chunked:
            inner = held & (chunk_rows - 1)
            block = (held >> inner_bits) & (count - 1)
            chunk = held >> (inner_bits + global_bits)
            held = inner + (chunk << inner_bits) + (block << low_bits)
        if swapped:
            low, high = held & (block_rows - 1), held >> low_bits
            index = low + (me << low_bits) + (high << row_bits)
        else:
            index = held + (me << row_bits)
        spin = (1 - 2 * ((index >> jnp.clip(lane_index - LANE_BITS, 0, 31)) & 1)).astype(F32)
        return jnp.where((lane_index >= LANE_BITS) & (lane_index < qubits), spin, 0.0)

    def field(spin, matrix, exact):
        if exact:
            half = mm(spin.astype(BF16), matrix.astype(BF16))
        else:
            half = mm_exact_left(spin.astype(BF16), matrix)
        half = jnp.where(lane_index < LANE_BITS, half, 0.5 * half * spin)
        lane_pairs = 0.5 * jnp.sum(
            mm_exact_right(matrix, lane_only.astype(BF16)) * lane_only, axis=0, keepdims=True
        )
        if exact:
            return mm(half.astype(BF16), lane_ones) + lane_pairs
        return mm_exact_right(half, lane_ones) + lane_pairs

    def copies(layer, chunk):
        return [
            pltpu.make_async_remote_copy(
                src_ref=send.at[layer, chunk, peers[step]],
                dst_ref=recv.at[layer, chunk, me],
                send_sem=send_sems.at[layer, chunk],
                recv_sem=recv_sems.at[layer, chunk],
                device_id={axis: peers[step]},
                device_id_type=MESH,
            )
            for step in plans[layer][chunk]
        ]

    def stat_copies(which):
        return [
            pltpu.make_async_remote_copy(
                src_ref=stat_send.at[which],
                dst_ref=stat_recv.at[which, me],
                send_sem=stat_send_sems.at[which],
                recv_sem=stat_recv_sems.at[which],
                device_id={axis: peers[step]},
                device_id_type=MESH,
            )
            for step in order
        ]

    others = pl.ds(0, count - 1)

    def blocks(layer, chunk):
        return pltpu.make_async_remote_copy(
            src_ref=send.at[layer, chunk, others],
            dst_ref=recv.at[layer, chunk, others],
            send_sem=send_sems.at[layer, chunk],
            recv_sem=recv_sems.at[layer, chunk],
            device_id={axis: peers[order[0]]},
            device_id_type=MESH,
        )

    def stats(which):
        return pltpu.make_async_remote_copy(
            src_ref=stat_recv.at[which, others],
            dst_ref=stat_recv.at[which, others],
            send_sem=stat_send_sems.at[which],
            recv_sem=stat_recv_sems.at[which],
            device_id={axis: peers[order[0]]},
            device_id_type=MESH,
        )

    def pack(layer, chunk, real, imag, first_row, stride):
        for block in range(count):
            start = first_row + block * stride
            part = slice(start, start + chunk_rows)
            send[layer, chunk, block, :chunk_rows, :] = real[part]
            send[layer, chunk, block, chunk_rows:, :] = imag[part]

    def received(layer, chunk):
        if chunk_rows % 8 == 0:
            return (
                jnp.concatenate([recv[layer, chunk, b, :chunk_rows, :] for b in range(count)], axis=0),
                jnp.concatenate([recv[layer, chunk, b, chunk_rows:, :] for b in range(count)], axis=0),
            )
        for block in range(count):
            part = slice(block * chunk_rows, (block + 1) * chunk_rows)
            plane_real[part, :] = recv[layer, chunk, block, :chunk_rows, :]
            plane_imag[part, :] = recv[layer, chunk, block, chunk_rows:, :]
        return plane_real[...], plane_imag[...]

    def part_of(values, chunk):
        return values[chunk * part_rows : (chunk + 1) * part_rows]

    def turned(real, imag, pairs):
        return apply_top(real, imag, pairs, chunk_rows)

    sine, cosine = sin_cos(field(row_spin(False, False), couplings([0])[0], False))
    lanes = lane_operand([turn(0, qubit) for qubit in range(LANE_BITS)])
    held = row_operand([turn(0, LANE_BITS + bit) for bit in range(row_bits)])

    arrivals[-1].wait()
    real = state_ref[pl.ds(0, rows, 2), :]
    imag = state_ref[pl.ds(1, rows, 2), :]
    stat_send[0] = jnp.sum(real * real + imag * imag, axis=0, keepdims=True)
    real, imag = cosine * real + sine * imag, cosine * imag - sine * real
    real, imag = apply_lanes(real, imag, lanes)
    real, imag = apply_rows(real, imag, held)
    first = [copies(0, chunk) for chunk in range(chunks)]
    second = [copies(1, chunk) for chunk in range(chunks)]
    norms, weights = stat_copies(0), stat_copies(1)
    for chunk in range(chunks):
        pack(0, chunk, real, imag, chunk * chunk_rows, block_rows)
    pl.semaphore_wait(barrier, count - 1)
    for copy in first[0]:
        copy.start()
    for chunk in range(chunks):
        recv[0, chunk, me] = send[0, chunk, me]
    stat_recv[0, me] = stat_send[0]

    moved = row_spin(True, True)
    next_bonds, sign_bonds = couplings([1, LAYERS])
    sine, cosine = sin_cos(field(moved, next_bonds, False))
    for chunk in range(1, chunks):
        blocks(0, chunk - 1).wait_send()
        for copy in first[chunk]:
            copy.start()
    for copy in norms:
        copy.start()
    lanes = lane_operand([turn(1, qubit) for qubit in range(LANE_BITS)])
    held = row_operand(
        [turn(1, LANE_BITS + bit) for bit in range(inner_bits)]
        + [turn(1, local_bits + bit) for bit in range(global_bits)]
    )
    late = [turn(1, LANE_BITS + inner_bits + bit) for bit in range(chunk_bits)]
    tops = [
        [turn(0, local_bits + bit) for bit in range(global_bits)],
        [turn(1, local_bits - global_bits + bit) for bit in range(global_bits)],
    ]
    energy_moved = field(moved, sign_bonds, True)
    energy_plain = field(row_spin(False, True), sign_bonds, True)

    between = []
    for chunk in range(chunks):
        blocks(0, chunk).wait_recv()
        real, imag = received(0, chunk)
        real, imag = turned(real, imag, tops[0])
        between.append((real, imag))
        part_sine, part_cosine = part_of(sine, chunk), part_of(cosine, chunk)
        real, imag = (
            part_cosine * real + part_sine * imag,
            part_cosine * imag - part_sine * real,
        )
        real, imag = apply_lanes(real, imag, lanes)
        real, imag = apply_rows(real, imag, held)
        pack(1, chunk, real, imag, 0, chunk_rows)
        for copy in second[chunk]:
            copy.start()
        recv[1, chunk, me] = send[1, chunk, me]

    def folded(parts, energy_field):
        total = jnp.zeros((1, LANES), F32)
        for chunk, (real, imag) in enumerate(parts):
            weight = (real * real + imag * imag) * part_of(energy_field, chunk)
            total = total + jnp.sum(weight, axis=0, keepdims=True)
        return total + pltpu.roll(total, LANES // 2, 1)

    energy_first = folded(between, energy_moved)
    stats(0).wait_recv()
    amps_total = F32(2.0**qubits)
    norm = jnp.sum(jnp.sum(stat_recv[0], axis=0), axis=1, keepdims=True)
    factor = 1.0 / jnp.sqrt(norm / amps_total + 1e-06)

    parts = []
    for chunk in range(chunks):
        blocks(1, chunk).wait_recv()
        real, imag = received(1, chunk)
        parts.append(turned(real, imag, tops[1]))
    for bit, (cosine, sine) in enumerate(late):
        fresh = list(parts)
        for low in range(chunks):
            high = low | 1 << bit
            if high == low:
                continue
            (low_real, low_imag), (high_real, high_imag) = parts[low], parts[high]
            fresh[low] = (cosine * low_real + sine * high_imag, cosine * low_imag - sine * high_real)
            fresh[high] = (cosine * high_real + sine * low_imag, cosine * high_imag - sine * low_real)
        parts = fresh

    lane = lax.broadcasted_iota(jnp.int32, (1, LANES), 1)
    stat_send[1] = jnp.where(lane < LANES // 2, energy_first, folded(parts, energy_plain))
    for copy in weights:
        copy.start()
    stat_recv[1, me] = stat_send[1]
    for chunk, (real, imag) in enumerate(parts):
        real, imag = real * factor, imag * factor
        for block in range(count):
            start = 2 * (block * block_rows + chunk * chunk_rows)
            part = slice(block * chunk_rows, (block + 1) * chunk_rows)
            out_ref[pl.ds(start, chunk_rows, 2), :] = real[part]
            out_ref[pl.ds(start + 1, chunk_rows, 2), :] = imag[part]
    blocks(0, chunks - 1).wait_send()
    for chunk in range(chunks):
        blocks(1, chunk).wait_send()
    stats(0).wait_send()
    stats(1).wait_recv()
    sums = jnp.sum(stat_recv[1], axis=0) * (factor * factor / amps_total)
    low_sum = jnp.sum(jnp.where(lane < LANES // 2, sums, 0.0), axis=1, keepdims=True)
    high_sum = jnp.sum(jnp.where(lane < LANES // 2, 0.0, sums), axis=1, keepdims=True)
    which = lax.broadcasted_iota(jnp.int32, (1, LAYERS), 1)
    energy_ref[...] = jnp.where(which == 0, low_sum, high_sum)
    stats(1).wait_send()


def place(state_ref, energy_ref, state_out, energy_out, sems):
    moves = [
        pltpu.make_async_copy(state_ref, state_out, sems.at[0]),
        pltpu.make_async_copy(energy_ref, energy_out, sems.at[1]),
    ]
    for move in moves:
        move.start()
    for move in moves:
        move.wait()


def solution(mesh):
    axis = "amp"
    count = mesh.shape[axis]

    def local(amplitudes, coupling_index, rotation_index, chain_order, bond_sign):
        rows = amplitudes.shape[1] // LANES
        qubits = chain_order.shape[0]
        block_rows = rows // count
        chunks = 2 if block_rows % 16 == 0 else 1
        chunk_rows = block_rows // chunks
        view = amplitudes.reshape(2, rows, LANES).transpose(1, 0, 2).reshape(2 * rows, LANES)
        vmem = pl.BlockSpec(memory_space=pltpu.VMEM)
        anywhere = pl.BlockSpec(memory_space=pl.ANY)
        state, energies = pl.pallas_call(
            functools.partial(kernel, axis, count, chunks, qubits),
            out_shape=(
                pltpu.VMEM((2 * rows, LANES), F32),
                pltpu.VMEM((1, LAYERS), F32),
            ),
            in_specs=[anywhere] * 5,
            out_specs=(vmem, vmem),
            scratch_shapes=[
                pltpu.VMEM((2 * rows, LANES), F32),
                pltpu.SMEM(coupling_index.shape, jnp.int32),
                pltpu.SMEM(rotation_index.shape, jnp.int32),
                pltpu.SMEM(chain_order.shape, jnp.int32),
                pltpu.SMEM(bond_sign.shape, jnp.int32),
                pltpu.SMEM((2, ANGLES), F32),
                pltpu.VMEM((LAYERS, chunks, count, 2 * chunk_rows, LANES), F32),
                pltpu.VMEM((LAYERS, chunks, count, 2 * chunk_rows, LANES), F32),
                pltpu.VMEM((2, 1, LANES), F32),
                pltpu.VMEM((2, count, 1, LANES), F32),
                pltpu.VMEM((rows, LANES), F32),
                pltpu.VMEM((rows, LANES), F32),
                pltpu.SemaphoreType.DMA((5,)),
                pltpu.SemaphoreType.DMA((LAYERS, chunks)),
                pltpu.SemaphoreType.DMA((LAYERS, chunks)),
                pltpu.SemaphoreType.DMA((2,)),
                pltpu.SemaphoreType.DMA((2,)),
            ],
            compiler_params=pltpu.CompilerParams(collective_id=0, has_side_effects=True),
        )(view, coupling_index, rotation_index, chain_order, bond_sign)
        state, energies = pl.pallas_call(
            place,
            out_shape=(
                jax.ShapeDtypeStruct((2 * rows, LANES), F32),
                jax.ShapeDtypeStruct((1, LAYERS), F32),
            ),
            in_specs=[anywhere] * 2,
            out_specs=(anywhere, anywhere),
            scratch_shapes=[pltpu.SemaphoreType.DMA((2,))],
        )(*(pltpu.with_memory_space_constraint(x, pltpu.VMEM) for x in (state, energies)))
        state = state.reshape(rows, 2, LANES).transpose(1, 0, 2).reshape(2, rows * LANES)
        return state, energies.reshape(LAYERS)

    in_specs = (P(None, ("rep", "amp")), P("rep", None), P("rep", None), P(), P())
    out_specs = (P(None, ("rep", "amp")), P("rep"))
    return jax.shard_map(local, mesh=mesh, in_specs=in_specs, out_specs=out_specs, check_vma=False)
```

```python
import functools
import math

import jax
import jax.numpy as jnp
from jax import lax
from jax.experimental import pallas as pl
from jax.experimental.pallas import tpu as pltpu
from jax.sharding import PartitionSpec as P

LAYERS = 2
ANGLES = 16
LANES = 128
LANE_BITS = 7
TILE = 8
F32 = jnp.float32
BF16 = jnp.bfloat16
MESH = pl.DeviceIdType.MESH
DOWN = (3, 2, 1, 0)
PLANS = (
    (((2, 3, 1, 0), (2, 0, 3, 1)), ((1, 0, 2, 3), DOWN)),
    (((2, 3, 1, 0), DOWN), ((2, 3, 0, 1), DOWN)),
)


def angle(index):
    return (index + 1).astype(F32) * F32(math.pi / (2.0 * (ANGLES + 1)))


def mm(left, right):
    return jnp.dot(left, right, preferred_element_type=F32)


def split(values):
    high = values.astype(BF16)
    return high, (values - high.astype(F32)).astype(BF16)


def mm3(left, right):
    return mm(left[0], right[0]) + mm(left[1], right[0]) + mm(left[0], right[1])


def mm_exact_left(left, values):
    high = values.astype(BF16)
    rest = values - high.astype(F32)
    middle = rest.astype(BF16)
    low = (rest - middle.astype(F32)).astype(BF16)
    return mm(left, high) + mm(left, middle) + mm(left, low)


def mm_exact_right(values, right):
    high = values.astype(BF16)
    rest = values - high.astype(F32)
    middle = rest.astype(BF16)
    low = (rest - middle.astype(F32)).astype(BF16)
    return mm(high, right) + mm(middle, right) + mm(low, right)


def sin_cos(values):
    turns = jnp.floor(values * F32(1.0 / math.pi) + 0.5)
    rest = values - turns * F32(3.140625)
    rest = rest - turns * F32(9.67502593994140625e-4)
    rest = rest - turns * F32(1.509957990978376432e-7)
    sign = 1.0 - 2.0 * (turns - 2.0 * jnp.floor(turns * 0.5))
    square = rest * rest
    sine = F32(-1.0 / 39916800)
    for coefficient in (1.0 / 362880, -1.0 / 5040, 1.0 / 120, -1.0 / 6, 1.0):
        sine = sine * square + F32(coefficient)
    cosine = F32(-1.0 / 3628800)
    for coefficient in (1.0 / 40320, -1.0 / 720, 1.0 / 24, -0.5, 1.0):
        cosine = cosine * square + F32(coefficient)
    return sine * (rest * sign), cosine * sign


def rotation(pairs, transposed=False):
    base = min(len(pairs), LANE_BITS)
    shape = (TILE, 2**base)
    row = lax.broadcasted_iota(jnp.int32, shape, 0)
    column = lax.broadcasted_iota(jnp.int32, shape, 1)

    def factors(bit):
        pair = pairs[bit]
        cosine, sine = (F32(1.0), F32(0.0)) if pair is None else pair
        if transposed:
            sine = -sine
        here = ((column >> bit) & 1) == 1
        return jnp.where(here, -sine, cosine), jnp.where(here, cosine, sine)

    value = None
    for bit in range(3):
        clear, put = factors(bit)
        factor = jnp.where(((row >> bit) & 1) == 1, put, clear)
        value = factor if value is None else value * factor
    found = [value]
    for bit in range(3, base):
        clear, put = factors(bit)
        found = [value * clear for value in found] + [value * put for value in found]
    value = jnp.concatenate(found, axis=0)
    for cosine, sine in pairs[base:]:
        value = jnp.concatenate(
            [
                jnp.concatenate([cosine * value, -sine * value], axis=1),
                jnp.concatenate([sine * value, cosine * value], axis=1),
            ],
            axis=0,
        )
    return value


def right_operand(matrix):
    high, low = split(matrix)
    return jnp.concatenate(
        [
            jnp.concatenate([high, low], axis=1),
            jnp.concatenate([high, jnp.zeros_like(high)], axis=1),
        ],
        axis=0,
    )


def paired(left, right):
    both = mm(left, right)
    return both[:, :LANES] + both[:, LANES:]


def apply_lanes(values, operand):
    return paired(jnp.concatenate(split(values), axis=1), operand)


def turn_blocks(values, pairs):
    height = values.shape[0]
    for bit, (cosine, sine) in enumerate(pairs):
        width = TILE << bit
        parts = []
        for start in range(0, height, 2 * width):
            low = values[start : start + width]
            high = values[start + width : start + 2 * width]
            parts += [cosine * low - sine * high, cosine * high + sine * low]
        values = jnp.concatenate(parts, axis=0)
    return values


def flipped(values):
    groups = values.reshape(values.shape[0] // TILE, TILE, LANES)
    return pltpu.roll(groups, TILE // 2, 1).reshape(values.shape)


def kernel(
    axis, count, chunks, depth, qubits,
    state_hbm, couple_hbm, turn_hbm, order_hbm, sign_hbm,
    out_ref, energy_ref,
    state_ref, couple_ref, turn_ref, order_ref, sign_ref,
    table, send, recv, norm_send, norm_recv, energy_send, energy_recv,
    local_sems, send_sem, recv_sems, stat_send_sems, stat_recv_sems, near_sem, far_sem,
):
    me = lax.axis_index(axis)
    rows = state_ref.shape[0] // 2
    row_bits = rows.bit_length() - 1
    global_bits = count.bit_length() - 1
    local_bits = row_bits + LANE_BITS
    block_rows = rows // count
    low_bits = row_bits - global_bits
    chunk_bits = chunks.bit_length() - 1
    chunk_rows = block_rows // chunks
    inner_bits = low_bits - chunk_bits
    tiles = rows // chunk_rows
    units = chunks // depth
    def ranked(groups, inner):
        size = count // 4
        steps = [
            group * size + high * (size // 4) + low
            for group in groups
            for high in inner
            for low in range(size // 4)
        ]
        return [step for step in steps if step]

    order = ranked((2, 3, 1, 0), (3, 2, 1, 0))
    plans = [[ranked(*plan) for plan in layer] for layer in PLANS]
    flips = [(1 - 2 * lax.rem(me // 2**bit, 2)) * 2**bit for bit in range(global_bits)]
    peers = {
        step: me + sum(flips[bit] for bit in range(global_bits) if step >> bit & 1)
        for step in order
    }

    quarter = count // 4
    top, second_bit = lax.div(me, 2 * quarter), lax.rem(lax.div(me, quarter), 2)
    middle = top + second_bit - 2 * top * second_bit
    inner = middle == 1
    outer = middle == 0

    def greet(semaphore, step):
        pl.semaphore_signal(
            semaphore, inc=1, device_id={axis: peers[step]}, device_id_type=MESH
        )

    barrier = pltpu.get_barrier_semaphore()

    @pl.when(inner)
    def _():
        for step in range(3 * quarter, count):
            greet(barrier, step)

    for step in range(2 * quarter - 1, 0, -1):
        greet(barrier, step)
    arrivals = [
        pltpu.make_async_copy(source, target, local_sems.at[number])
        for number, (source, target) in enumerate(
            [
                (couple_hbm, couple_ref),
                (turn_hbm, turn_ref),
                (order_hbm, order_ref),
                (sign_hbm, sign_ref),
                (state_hbm, state_ref),
            ]
        )
    ]
    for copy in arrivals:
        copy.start()


    for entry in range(ANGLES):
        theta = (entry + 1) * math.pi / (2.0 * (ANGLES + 1))
        table[0, entry] = F32(math.cos(theta))
        table[1, entry] = F32(math.sin(theta))
    for copy in arrivals[:-1]:
        copy.wait()

    def turn(layer, qubit):
        index = turn_ref[layer, qubit]
        return table[0, index], table[1, index]

    height = -(-qubits // 8) * 8
    place = lax.broadcasted_iota(jnp.int32, (height, LANES), 0) * LANES + (
        lax.broadcasted_iota(jnp.int32, (height, LANES), 1)
    )

    def couplings(layers):
        matrices = [jnp.zeros((height, LANES), F32) for _ in layers]
        for bond in range(qubits - 1):
            start, end = order_ref[bond], order_ref[bond + 1]
            here = (place == start * LANES + end) | (place == end * LANES + start)
            for number, layer in enumerate(layers):
                value = (2 * sign_ref[bond] - 1).astype(F32)
                if layer < LAYERS:
                    value = angle(couple_ref[layer, bond]) * value
                matrices[number] = jnp.where(here, value, matrices[number])
        rest = jnp.zeros((LANES - height, LANES), F32)
        return [jnp.concatenate([matrix, rest], axis=0) for matrix in matrices]

    square_row = lax.broadcasted_iota(jnp.int32, (LANES, LANES), 0)
    square_lane = lax.broadcasted_iota(jnp.int32, (LANES, LANES), 1)
    lane_spin = (1 - 2 * ((square_lane >> jnp.minimum(square_row, 31)) & 1)).astype(F32)
    lane_only = jnp.where(square_row < LANE_BITS, lane_spin, 0.0)
    lane_ones = jnp.where(square_row < LANE_BITS, lane_spin, 1.0).astype(BF16)
    row_index = lax.broadcasted_iota(jnp.int32, (rows, LANES), 0)
    lane_index = lax.broadcasted_iota(jnp.int32, (rows, LANES), 1)

    def row_spin(swapped, chunked):
        held = row_index
        if chunked:
            inner = held & (chunk_rows - 1)
            block = (held >> inner_bits) & (count - 1)
            chunk = held >> (inner_bits + global_bits)
            held = inner + (chunk << inner_bits) + (block << low_bits)
        if swapped:
            low, high = held & (block_rows - 1), held >> low_bits
            index = low + (me << low_bits) + (high << row_bits)
        else:
            index = held + (me << row_bits)
        spin = (1 - 2 * ((index >> jnp.clip(lane_index - LANE_BITS, 0, 31)) & 1)).astype(F32)
        return jnp.where((lane_index >= LANE_BITS) & (lane_index < qubits), spin, 0.0)

    def field(spin, matrix, exact, half=None):
        if half is not None:
            pass
        elif exact:
            half = mm(spin.astype(BF16), matrix.astype(BF16))
        else:
            half = mm_exact_left(spin.astype(BF16), matrix)
        half = jnp.where(lane_index < LANE_BITS, half, 0.5 * half * spin)
        lane_pairs = 0.5 * jnp.sum(
            mm_exact_right(matrix[:TILE], lane_only.astype(BF16)) * lane_only[:TILE],
            axis=0,
            keepdims=True,
        )
        if exact:
            return mm(half.astype(BF16), lane_ones) + lane_pairs
        return mm_exact_right(half, lane_ones) + lane_pairs

    def copies(layer, unit, steps=None):
        return [
            pltpu.make_async_remote_copy(
                src_ref=send.at[layer, unit, peers[step]],
                dst_ref=recv.at[layer, unit, me],
                send_sem=send_sem,
                recv_sem=recv_sems.at[layer, unit],
                device_id={axis: peers[step]},
                device_id_type=MESH,
            )
            for step in (plans[layer][unit % 2] if steps is None else steps)
        ]

    def stat_copies(which):
        return [
            pltpu.make_async_remote_copy(
                src_ref=(norm_send, energy_send)[which],
                dst_ref=(norm_recv, energy_recv)[which].at[me],
                send_sem=stat_send_sems.at[which],
                recv_sem=stat_recv_sems.at[which],
                device_id={axis: peers[step]},
                device_id_type=MESH,
            )
            for step in order
        ]

    others = pl.ds(0, count - 1)

    def blocks(layer, unit):
        return pltpu.make_async_remote_copy(
            src_ref=send.at[layer, unit, others],
            dst_ref=recv.at[layer, unit, others],
            send_sem=send_sem,
            recv_sem=recv_sems.at[layer, unit],
            device_id={axis: peers[order[0]]},
            device_id_type=MESH,
        )

    def shelf(chunk):
        start = chunk % depth * TILE
        return slice(start, start + TILE)

    def received(layer, chunk):
        values = recv[layer, chunk // depth, :, shelf(chunk), :]
        return values.reshape(count * TILE, LANES)

    def stats(which):
        return pltpu.make_async_remote_copy(
            src_ref=(norm_recv, energy_recv)[which].at[others],
            dst_ref=(norm_recv, energy_recv)[which].at[others],
            send_sem=stat_send_sems.at[which],
            recv_sem=stat_recv_sems.at[which],
            device_id={axis: peers[order[0]]},
            device_id_type=MESH,
        )

    upper = lax.broadcasted_iota(jnp.int32, (TILE, LANES), 0) < TILE // 2
    side = jnp.where(upper, F32(1.0), F32(-1.0))

    def tile(values, number):
        return values[number * TILE : (number + 1) * TILE]

    def spread(values, signed):
        turned = flipped(values)
        found = []
        for number in range(tiles):
            here, there = tile(values, number // 2), tile(turned, number // 2)
            if number % 2:
                here, there = there, here
            both = jnp.where(upper, here, there)
            found.append(both * side if signed else both)
        return found

    def part(found, chunk):
        return jnp.concatenate(found[chunk * count : (chunk + 1) * count], axis=0)

    def ones(values, bits):
        return sum((values >> bit) & 1 for bit in range(bits))

    small_row = lax.broadcasted_iota(jnp.int32, (TILE, LANES), 0)
    small_lane = lax.broadcasted_iota(jnp.int32, (TILE, LANES), 1)
    held_ones = ones(small_lane, LANE_BITS) + sum(
        lax.rem(lax.div(me, 2**bit), 2) for bit in range(global_bits)
    )
    quarters = [
        ((held_ones + ones(small_row, 3) + more) & 3).astype(F32) * F32(-math.pi / 2)
        for more in range(4)
    ]
    frame = jnp.concatenate(
        [quarters[number.bit_count() & 3] for number in range(rows // TILE)], axis=0
    )

    def doubled(first, step):
        found = [first]
        for bit in range(3, row_bits):
            found = sum(zip(*[step(value, bit) for value in found]), ())
        return jnp.concatenate(found, axis=0)

    def own_spin(bit):
        if bit < row_bits:
            return (1 - 2 * ((small_row >> bit) & 1)).astype(F32)
        bit = bit - row_bits
        return (1 - 2 * lax.rem(lax.div(me, 2**bit), 2)).astype(F32)

    own_bits = list(range(3)) + list(range(row_bits, row_bits + global_bits))
    above = small_lane - LANE_BITS
    first_spin = jnp.where((above >= 0) & (above < row_bits), F32(1.0), F32(0.0))
    for bit in own_bits:
        first_spin = jnp.where(above == bit, own_spin(bit), first_spin)
    bonds = couplings([0])[0]

    def bond_row(bit):
        return bonds[LANE_BITS + bit : LANE_BITS + bit + 1]

    spin = doubled(
        first_spin,
        lambda value, bit: (value, jnp.where(above == bit, -value, value)),
    )
    half = doubled(
        sum(own_spin(bit) * bond_row(bit) for bit in own_bits),
        lambda value, bit: (value + bond_row(bit), value - bond_row(bit)),
    )
    sine, cosine = sin_cos(field(spin, bonds, False, half) + frame)
    lanes = right_operand(rotation([turn(0, qubit) for qubit in range(LANE_BITS)], True))
    held = split(rotation([turn(0, LANE_BITS + bit) for bit in range(row_bits)]))

    arrivals[-1].wait()
    real = state_ref[pl.ds(0, rows, 2), :]
    imag = state_ref[pl.ds(1, rows, 2), :]
    norm_send[...] = jnp.sum(real * real + imag * imag, axis=0, keepdims=True)
    real, imag = cosine * real + sine * imag, cosine * imag - sine * real
    both = apply_lanes(jnp.concatenate([real, imag], axis=0), lanes)
    both = mm3(held, split(jnp.concatenate([both[:rows], both[rows:]], axis=1)))
    real, imag = both[:, :LANES], both[:, LANES:]
    turned_real, turned_imag = flipped(real), flipped(imag)
    first = [copies(0, unit) if unit else [] for unit in range(units)]
    second = [copies(1, unit) for unit in range(units)]
    norms, weights = stat_copies(0), stat_copies(1)
    def pack(unit):
        for chunk in range(unit * depth, unit * depth + depth):
            for block in range(count):
                number = block * chunks + chunk
                if number % 2:
                    ends = tile(turned_real, number // 2), tile(imag, number // 2)
                else:
                    ends = tile(real, number // 2), tile(turned_imag, number // 2)
                send[0, unit, block, shelf(chunk), :] = jnp.where(upper, *ends)

    pack(0)
    def begin(groups):
        for group in groups:
            steps = [group * quarter + low for low in reversed(range(quarter))]
            for copy in copies(0, 0, [step for step in steps if step]):
                copy.start()

    pl.semaphore_wait(barrier, 2 * quarter - 1 + middle * quarter)

    @pl.when(inner)
    def _():
        greet(near_sem, 3 * quarter)
        greet(near_sem, quarter)
        begin((3,))

    begin((1, 0))
    for unit in range(1, units):
        pack(unit)
    pl.semaphore_wait(near_sem, 1)

    @pl.when(inner)
    def _():
        greet(far_sem, quarter)
        begin((2,))

    @pl.when(outer)
    def _():
        begin((2,))
        pl.semaphore_wait(far_sem, 1)
        begin((3,))

    for unit in range(units):
        recv[0, unit, me] = send[0, unit, me]
    norm_recv[me] = norm_send[...]

    moved = row_spin(True, True)
    next_bonds, sign_bonds = couplings([1, LAYERS])
    sine, cosine = sin_cos(field(moved, next_bonds, False))
    sine, cosine = spread(sine, True), spread(cosine, False)
    for unit in range(1, units):
        for copy in first[unit]:
            copy.start()
    for copy in norms:
        copy.start()
    lanes = right_operand(rotation([turn(1, qubit) for qubit in range(LANE_BITS)], True))
    held = jnp.concatenate(
        split(
            rotation(
                [turn(1, LANE_BITS + bit) for bit in range(inner_bits)]
                + [None]
                + [turn(1, local_bits + bit) for bit in range(global_bits)]
            )
        ),
        axis=1,
    )
    late = [turn(1, LANE_BITS + inner_bits + bit) for bit in range(chunk_bits)]
    tops = [
        [turn(0, local_bits + bit) for bit in range(global_bits)],
        [turn(1, local_bits - global_bits + bit) for bit in range(global_bits)],
    ]
    energy_moved = spread(field(moved, sign_bonds, True), False)
    energy_plain = spread(field(row_spin(False, True), sign_bonds, True), False)

    def folded(parts, energy_field):
        total = jnp.zeros((TILE, LANES), F32)
        for chunk, values in enumerate(parts):
            weight = values * values * part(energy_field, chunk)
            for block in range(count):
                total = total + tile(weight, block)
        return jnp.sum(total, axis=0, keepdims=True)

    between = []
    for chunk in range(chunks):
        if chunk % depth == 0:
            blocks(0, chunk // depth).wait_recv()
        values = turn_blocks(received(0, chunk), tops[0])
        between.append(values)
        values = part(cosine, chunk) * values + part(sine, chunk) * flipped(values)
        values = apply_lanes(values, lanes)
        values = paired(held, right_operand(values))
        unit = chunk // depth
        send[1, unit, :, shelf(chunk), :] = values.reshape(count, TILE, LANES)
        if chunk % depth == depth - 1:
            for copy in second[unit]:
                copy.start()
            recv[1, unit, me] = send[1, unit, me]

    energy_send[0:1] = folded(between, energy_moved)
    stats(0).wait_recv()
    amps_total = F32(2.0**qubits)
    norm = jnp.sum(jnp.sum(norm_recv[...], axis=0), axis=1, keepdims=True)
    factor = 1.0 / jnp.sqrt(norm / amps_total + 1e-06)
    phase = (held_ones + ones(small_row, inner_bits)) & 3
    even = (phase & 1) == 0
    sign = jnp.where((phase & 2) == 0, factor, -factor)
    along, across = jnp.where(even, sign, 0.0), jnp.where(even, 0.0, sign)
    frames = [
        (along, across * side),
        (-across, along * side),
        (-along, -across * side),
        (across, -along * side),
    ]

    parts = []
    for chunk in range(chunks):
        if chunk % depth == 0:
            blocks(1, chunk // depth).wait_recv()
        parts.append(turn_blocks(received(1, chunk), tops[1]))
        for bit, (cosine, sine) in enumerate(late):
            if (chunk + 1) % (2 << bit) == 0:
                for high in range(chunk + 1 - (1 << bit), chunk + 1):
                    low = high - (1 << bit)
                    parts[low], parts[high] = (
                        cosine * parts[low] - sine * parts[high],
                        cosine * parts[high] + sine * parts[low],
                    )

    energy_send[1:2] = folded(parts, energy_plain)
    for copy in weights:
        copy.start()
    energy_recv[me] = energy_send[...]
    for chunk, values in enumerate(parts):
        turned = flipped(values)
        for block in range(count):
            along, across = frames[(block.bit_count() + chunk.bit_count()) & 3]
            final = along * tile(values, block) + across * tile(turned, block)
            start = TILE * (block * chunks + chunk)
            out_ref[pl.ds(start, chunk_rows, 2), :] = final[:chunk_rows]
            out_ref[pl.ds(start + 1, chunk_rows, 2), :] = final[chunk_rows:]
    pltpu.make_async_remote_copy(
        src_ref=send.at[:, :, others],
        dst_ref=recv.at[:, :, others],
        send_sem=send_sem,
        recv_sem=recv_sems.at[0, 0],
        device_id={axis: peers[order[0]]},
        device_id_type=MESH,
    ).wait_send()
    stats(0).wait_send()
    stats(1).wait_recv()
    sums = jnp.sum(energy_recv[...], axis=0) * (factor * factor / amps_total)
    sums = jnp.sum(sums, axis=1, keepdims=True)
    which = lax.broadcasted_iota(jnp.int32, (1, LAYERS), 1)
    energy_ref[...] = jnp.where(which == 0, sums[0:1], sums[1:2])
    stats(1).wait_send()


def place(state_ref, energy_ref, state_out, energy_out, sems):
    moves = [
        pltpu.make_async_copy(state_ref, state_out, sems.at[0]),
        pltpu.make_async_copy(energy_ref, energy_out, sems.at[1]),
    ]
    for move in moves:
        move.start()
    for move in moves:
        move.wait()


def solution(mesh):
    axis = "amp"
    count = mesh.shape[axis]

    def local(amplitudes, coupling_index, rotation_index, chain_order, bond_sign):
        rows = amplitudes.shape[1] // LANES
        qubits = chain_order.shape[0]
        block_rows = rows // count
        chunk_rows = TILE // 2
        chunks = block_rows // chunk_rows
        depth = 2 if chunks % 2 == 0 else 1
        units = chunks // depth
        view = amplitudes.reshape(2, rows, LANES).transpose(1, 0, 2).reshape(2 * rows, LANES)
        vmem = pl.BlockSpec(memory_space=pltpu.VMEM)
        anywhere = pl.BlockSpec(memory_space=pl.ANY)
        state, energies = pl.pallas_call(
            functools.partial(kernel, axis, count, chunks, depth, qubits),
            out_shape=(
                pltpu.VMEM((2 * rows, LANES), F32),
                pltpu.VMEM((1, LAYERS), F32),
            ),
            in_specs=[anywhere] * 5,
            out_specs=(vmem, vmem),
            scratch_shapes=[
                pltpu.VMEM((2 * rows, LANES), F32),
                pltpu.SMEM(coupling_index.shape, jnp.int32),
                pltpu.SMEM(rotation_index.shape, jnp.int32),
                pltpu.SMEM(chain_order.shape, jnp.int32),
                pltpu.SMEM(bond_sign.shape, jnp.int32),
                pltpu.SMEM((2, ANGLES), F32),
                pltpu.VMEM((LAYERS, units, count, depth * TILE, LANES), F32),
                pltpu.VMEM((LAYERS, units, count, depth * TILE, LANES), F32),
                pltpu.VMEM((1, LANES), F32),
                pltpu.VMEM((count, 1, LANES), F32),
                pltpu.VMEM((LAYERS, LANES), F32),
                pltpu.VMEM((count, LAYERS, LANES), F32),
                pltpu.SemaphoreType.DMA((5,)),
                pltpu.SemaphoreType.DMA,
                pltpu.SemaphoreType.DMA((LAYERS, units)),
                pltpu.SemaphoreType.DMA((2,)),
                pltpu.SemaphoreType.DMA((2,)),
                pltpu.SemaphoreType.REGULAR,
                pltpu.SemaphoreType.REGULAR,
            ],
            compiler_params=pltpu.CompilerParams(collective_id=0, has_side_effects=True),
        )(view, coupling_index, rotation_index, chain_order, bond_sign)
        state, energies = pl.pallas_call(
            place,
            out_shape=(
                jax.ShapeDtypeStruct((2 * rows, LANES), F32),
                jax.ShapeDtypeStruct((1, LAYERS), F32),
            ),
            in_specs=[anywhere] * 2,
            out_specs=(anywhere, anywhere),
            scratch_shapes=[pltpu.SemaphoreType.DMA((2,))],
        )(*(pltpu.with_memory_space_constraint(x, pltpu.VMEM) for x in (state, energies)))
        state = state.reshape(rows, 2, LANES).transpose(1, 0, 2).reshape(2, rows * LANES)
        return state, energies.reshape(LAYERS)

    in_specs = (P(None, ("rep", "amp")), P("rep", None), P("rep", None), P(), P())
    out_specs = (P(None, ("rep", "amp")), P("rep"))
    return jax.shard_map(local, mesh=mesh, in_specs=in_specs, out_specs=out_specs, check_vma=False)
```

```python
import functools
import math

import jax
import jax.numpy as jnp
from jax import lax
from jax.experimental import pallas as pl
from jax.experimental.pallas import tpu as pltpu
from jax.sharding import PartitionSpec as P

LAYERS = 2
ANGLES = 16
LANES = 128
LANE_BITS = 7
TILE = 8
F32 = jnp.float32
BF16 = jnp.bfloat16
MESH = pl.DeviceIdType.MESH
DOWN = (3, 2, 1, 0)
PLANS = (
    (((2, 3, 1, 0), DOWN), ((1, 0, 2, 3), DOWN)),
    (((2, 1, 3, 0), DOWN), ((2, 3, 0, 1), DOWN)),
)
INNER = (
    (((2, 3, 1, 0), DOWN), ((1, 0, 2, 3), DOWN)),
    (((2, 3, 1, 0), DOWN), ((2, 3, 0, 1), DOWN)),
)


def angle(index):
    return (index + 1).astype(F32) * F32(math.pi / (2.0 * (ANGLES + 1)))


def mm(left, right):
    return jnp.dot(left, right, preferred_element_type=F32)


def split(values):
    high = values.astype(BF16)
    return high, (values - high.astype(F32)).astype(BF16)


def mm3(left, right):
    return mm(left[0], right[0]) + mm(left[1], right[0]) + mm(left[0], right[1])


def mm_exact_left(left, values):
    high = values.astype(BF16)
    rest = values - high.astype(F32)
    middle = rest.astype(BF16)
    low = (rest - middle.astype(F32)).astype(BF16)
    return mm(left, high) + mm(left, middle) + mm(left, low)


def mm_exact_right(values, right):
    high = values.astype(BF16)
    rest = values - high.astype(F32)
    middle = rest.astype(BF16)
    low = (rest - middle.astype(F32)).astype(BF16)
    return mm(high, right) + mm(middle, right) + mm(low, right)


def sin_cos(values):
    turns = jnp.floor(values * F32(1.0 / math.pi) + 0.5)
    rest = values - turns * F32(3.140625)
    rest = rest - turns * F32(9.67502593994140625e-4)
    rest = rest - turns * F32(1.509957990978376432e-7)
    sign = 1.0 - 2.0 * (turns - 2.0 * jnp.floor(turns * 0.5))
    square = rest * rest
    sine = F32(-1.0 / 39916800)
    for coefficient in (1.0 / 362880, -1.0 / 5040, 1.0 / 120, -1.0 / 6, 1.0):
        sine = sine * square + F32(coefficient)
    cosine = F32(-1.0 / 3628800)
    for coefficient in (1.0 / 40320, -1.0 / 720, 1.0 / 24, -0.5, 1.0):
        cosine = cosine * square + F32(coefficient)
    return sine * (rest * sign), cosine * sign


def rotation(pairs, transposed=False):
    base = min(len(pairs), LANE_BITS)
    shape = (TILE, 2**base)
    row = lax.broadcasted_iota(jnp.int32, shape, 0)
    column = lax.broadcasted_iota(jnp.int32, shape, 1)

    def factors(bit):
        pair = pairs[bit]
        cosine, sine = (F32(1.0), F32(0.0)) if pair is None else pair
        if transposed:
            sine = -sine
        here = ((column >> bit) & 1) == 1
        return jnp.where(here, -sine, cosine), jnp.where(here, cosine, sine)

    value = None
    for bit in range(3):
        clear, put = factors(bit)
        factor = jnp.where(((row >> bit) & 1) == 1, put, clear)
        value = factor if value is None else value * factor
    found = [value]
    for bit in range(3, base):
        clear, put = factors(bit)
        found = [value * clear for value in found] + [value * put for value in found]
    value = jnp.concatenate(found, axis=0)
    for cosine, sine in pairs[base:]:
        value = jnp.concatenate(
            [
                jnp.concatenate([cosine * value, -sine * value], axis=1),
                jnp.concatenate([sine * value, cosine * value], axis=1),
            ],
            axis=0,
        )
    return value


def right_operand(matrix):
    high, low = split(matrix)
    return jnp.concatenate(
        [
            jnp.concatenate([high, low], axis=1),
            jnp.concatenate([high, jnp.zeros_like(high)], axis=1),
        ],
        axis=0,
    )


def paired(left, right):
    both = mm(left, right)
    return both[:, :LANES] + both[:, LANES:]


def apply_lanes(values, operand):
    return paired(jnp.concatenate(split(values), axis=1), operand)


def turn_blocks(values, pairs):
    height = values.shape[0]
    for bit, (cosine, sine) in enumerate(pairs):
        width = TILE << bit
        parts = []
        for start in range(0, height, 2 * width):
            low = values[start : start + width]
            high = values[start + width : start + 2 * width]
            parts += [cosine * low - sine * high, cosine * high + sine * low]
        values = jnp.concatenate(parts, axis=0)
    return values


def flipped(values):
    groups = values.reshape(values.shape[0] // TILE, TILE, LANES)
    return pltpu.roll(groups, TILE // 2, 1).reshape(values.shape)


def kernel(
    axis, count, chunks, depth, qubits,
    state_hbm, couple_hbm, turn_hbm, order_hbm, sign_hbm,
    out_ref, energy_ref,
    state_ref, couple_ref, turn_ref, order_ref, sign_ref,
    table, send, recv, norm_send, norm_recv, energy_send, energy_recv,
    local_sems, send_sem, recv_sems, stat_send_sems, stat_recv_sems, near_sem, far_sem,
):
    me = lax.axis_index(axis)
    rows = state_ref.shape[0] // 2
    row_bits = rows.bit_length() - 1
    global_bits = count.bit_length() - 1
    local_bits = row_bits + LANE_BITS
    block_rows = rows // count
    low_bits = row_bits - global_bits
    chunk_bits = chunks.bit_length() - 1
    chunk_rows = block_rows // chunks
    inner_bits = low_bits - chunk_bits
    tiles = rows // chunk_rows
    units = chunks // depth
    def ranked(groups, inner):
        size = count // 4
        steps = [
            group * size + high * (size // 4) + low
            for group in groups
            for high in inner
            for low in range(size // 4)
        ]
        return [step for step in steps if step]

    order = ranked((2, 3, 1, 0), (3, 2, 1, 0))
    flips = [(1 - 2 * lax.rem(me // 2**bit, 2)) * 2**bit for bit in range(global_bits)]
    peers = {
        step: me + sum(flips[bit] for bit in range(global_bits) if step >> bit & 1)
        for step in order
    }

    quarter = count // 4
    top, second_bit = lax.div(me, 2 * quarter), lax.rem(lax.div(me, quarter), 2)
    middle = top + second_bit - 2 * top * second_bit
    inner = middle == 1
    outer = middle == 0

    def greet(semaphore, step):
        pl.semaphore_signal(
            semaphore, inc=1, device_id={axis: peers[step]}, device_id_type=MESH
        )

    barrier = pltpu.get_barrier_semaphore()

    @pl.when(inner)
    def _():
        for step in range(3 * quarter, count):
            greet(barrier, step)

    for step in range(2 * quarter - 1, 0, -1):
        greet(barrier, step)
    arrivals = [
        pltpu.make_async_copy(source, target, local_sems.at[number])
        for number, (source, target) in enumerate(
            [
                (couple_hbm, couple_ref),
                (turn_hbm, turn_ref),
                (order_hbm, order_ref),
                (sign_hbm, sign_ref),
                (state_hbm, state_ref),
            ]
        )
    ]
    for copy in arrivals:
        copy.start()


    for entry in range(ANGLES):
        theta = (entry + 1) * math.pi / (2.0 * (ANGLES + 1))
        table[0, entry] = F32(math.cos(theta))
        table[1, entry] = F32(math.sin(theta))
    for copy in arrivals[:-1]:
        copy.wait()

    def turn(layer, qubit):
        index = turn_ref[layer, qubit]
        return table[0, index], table[1, index]

    height = -(-qubits // 8) * 8
    place = lax.broadcasted_iota(jnp.int32, (height, LANES), 0) * LANES + (
        lax.broadcasted_iota(jnp.int32, (height, LANES), 1)
    )

    def couplings(layers):
        matrices = [jnp.zeros((height, LANES), F32) for _ in layers]
        for bond in range(qubits - 1):
            start, end = order_ref[bond], order_ref[bond + 1]
            here = (place == start * LANES + end) | (place == end * LANES + start)
            for number, layer in enumerate(layers):
                value = (2 * sign_ref[bond] - 1).astype(F32)
                if layer < LAYERS:
                    value = angle(couple_ref[layer, bond]) * value
                matrices[number] = jnp.where(here, value, matrices[number])
        rest = jnp.zeros((LANES - height, LANES), F32)
        return [jnp.concatenate([matrix, rest], axis=0) for matrix in matrices]

    square_row = lax.broadcasted_iota(jnp.int32, (LANES, LANES), 0)
    square_lane = lax.broadcasted_iota(jnp.int32, (LANES, LANES), 1)
    lane_spin = (1 - 2 * ((square_lane >> jnp.minimum(square_row, 31)) & 1)).astype(F32)
    lane_only = jnp.where(square_row < LANE_BITS, lane_spin, 0.0)
    lane_ones = jnp.where(square_row < LANE_BITS, lane_spin, 1.0).astype(BF16)
    row_index = lax.broadcasted_iota(jnp.int32, (rows, LANES), 0)
    lane_index = lax.broadcasted_iota(jnp.int32, (rows, LANES), 1)

    def row_spin(swapped, chunked):
        held = row_index
        if chunked:
            inner = held & (chunk_rows - 1)
            block = (held >> inner_bits) & (count - 1)
            chunk = held >> (inner_bits + global_bits)
            held = inner + (chunk << inner_bits) + (block << low_bits)
        if swapped:
            low, high = held & (block_rows - 1), held >> low_bits
            index = low + (me << low_bits) + (high << row_bits)
        else:
            index = held + (me << row_bits)
        spin = (1 - 2 * ((index >> jnp.clip(lane_index - LANE_BITS, 0, 31)) & 1)).astype(F32)
        return jnp.where((lane_index >= LANE_BITS) & (lane_index < qubits), spin, 0.0)

    def field(spin, matrix, exact, half=None):
        if half is not None:
            pass
        elif exact:
            half = mm(spin.astype(BF16), matrix.astype(BF16))
        else:
            half = mm_exact_left(spin.astype(BF16), matrix)
        half = jnp.where(lane_index < LANE_BITS, half, 0.5 * half * spin)
        lane_pairs = 0.5 * jnp.sum(
            mm_exact_right(matrix[:TILE], lane_only.astype(BF16)) * lane_only[:TILE],
            axis=0,
            keepdims=True,
        )
        if exact:
            return mm(half.astype(BF16), lane_ones) + lane_pairs
        return mm_exact_right(half, lane_ones) + lane_pairs

    def copies(layer, unit, steps):
        return [
            pltpu.make_async_remote_copy(
                src_ref=send.at[layer, unit, peers[step]],
                dst_ref=recv.at[layer, unit, me],
                send_sem=send_sem,
                recv_sem=recv_sems.at[layer, unit],
                device_id={axis: peers[step]},
                device_id_type=MESH,
            )
            for step in steps
        ]

    def stat_copies(which):
        return [
            pltpu.make_async_remote_copy(
                src_ref=(norm_send, energy_send)[which],
                dst_ref=(norm_recv, energy_recv)[which].at[me],
                send_sem=stat_send_sems.at[which],
                recv_sem=stat_recv_sems.at[which],
                device_id={axis: peers[step]},
                device_id_type=MESH,
            )
            for step in order
        ]

    others = pl.ds(0, count - 1)

    def blocks(layer, unit):
        return pltpu.make_async_remote_copy(
            src_ref=send.at[layer, unit, others],
            dst_ref=recv.at[layer, unit, others],
            send_sem=send_sem,
            recv_sem=recv_sems.at[layer, unit],
            device_id={axis: peers[order[0]]},
            device_id_type=MESH,
        )

    def shelf(chunk):
        start = chunk % depth * TILE
        return slice(start, start + TILE)

    def received(layer, chunk):
        values = recv[layer, chunk // depth, :, shelf(chunk), :]
        return values.reshape(count * TILE, LANES)

    def stats(which):
        return pltpu.make_async_remote_copy(
            src_ref=(norm_recv, energy_recv)[which].at[others],
            dst_ref=(norm_recv, energy_recv)[which].at[others],
            send_sem=stat_send_sems.at[which],
            recv_sem=stat_recv_sems.at[which],
            device_id={axis: peers[order[0]]},
            device_id_type=MESH,
        )

    upper = lax.broadcasted_iota(jnp.int32, (TILE, LANES), 0) < TILE // 2
    side = jnp.where(upper, F32(1.0), F32(-1.0))

    def tile(values, number):
        return values[number * TILE : (number + 1) * TILE]

    def spread(values, signed):
        turned = flipped(values)
        found = []
        for number in range(tiles):
            here, there = tile(values, number // 2), tile(turned, number // 2)
            if number % 2:
                here, there = there, here
            both = jnp.where(upper, here, there)
            found.append(both * side if signed else both)
        return found

    def part(found, chunk):
        return jnp.concatenate(found[chunk * count : (chunk + 1) * count], axis=0)

    def ones(values, bits):
        return sum((values >> bit) & 1 for bit in range(bits))

    small_row = lax.broadcasted_iota(jnp.int32, (TILE, LANES), 0)
    small_lane = lax.broadcasted_iota(jnp.int32, (TILE, LANES), 1)
    held_ones = ones(small_lane, LANE_BITS) + sum(
        lax.rem(lax.div(me, 2**bit), 2) for bit in range(global_bits)
    )
    quarters = [
        ((held_ones + ones(small_row, 3) + more) & 3).astype(F32) * F32(-math.pi / 2)
        for more in range(4)
    ]
    frame = jnp.concatenate(
        [quarters[number.bit_count() & 3] for number in range(rows // TILE)], axis=0
    )

    def doubled(first, step):
        found = [first]
        for bit in range(3, row_bits):
            found = sum(zip(*[step(value, bit) for value in found]), ())
        return jnp.concatenate(found, axis=0)

    def own_spin(bit):
        if bit < row_bits:
            return (1 - 2 * ((small_row >> bit) & 1)).astype(F32)
        bit = bit - row_bits
        return (1 - 2 * lax.rem(lax.div(me, 2**bit), 2)).astype(F32)

    own_bits = list(range(3)) + list(range(row_bits, row_bits + global_bits))
    above = small_lane - LANE_BITS
    first_spin = jnp.where((above >= 0) & (above < row_bits), F32(1.0), F32(0.0))
    for bit in own_bits:
        first_spin = jnp.where(above == bit, own_spin(bit), first_spin)
    bonds = couplings([0])[0]

    def bond_row(bit):
        return bonds[LANE_BITS + bit : LANE_BITS + bit + 1]

    spin = doubled(
        first_spin,
        lambda value, bit: (value, jnp.where(above == bit, -value, value)),
    )
    half = doubled(
        sum(own_spin(bit) * bond_row(bit) for bit in own_bits),
        lambda value, bit: (value + bond_row(bit), value - bond_row(bit)),
    )
    sine, cosine = sin_cos(field(spin, bonds, False, half) + frame)
    lanes = right_operand(rotation([turn(0, qubit) for qubit in range(LANE_BITS)], True))
    held = split(rotation([turn(0, LANE_BITS + bit) for bit in range(row_bits)]))

    arrivals[-1].wait()
    real = state_ref[pl.ds(0, rows, 2), :]
    imag = state_ref[pl.ds(1, rows, 2), :]
    norm_send[...] = jnp.sum(real * real + imag * imag, axis=0, keepdims=True)
    real, imag = cosine * real + sine * imag, cosine * imag - sine * real
    both = apply_lanes(jnp.concatenate([real, imag], axis=0), lanes)
    both = mm3(held, split(jnp.concatenate([both[:rows], both[rows:]], axis=1)))
    real, imag = both[:, :LANES], both[:, LANES:]
    turned_real, turned_imag = flipped(real), flipped(imag)
    norms, weights = stat_copies(0), stat_copies(1)
    def pack(unit):
        for chunk in range(unit * depth, unit * depth + depth):
            for block in range(count):
                number = block * chunks + chunk
                if number % 2:
                    ends = tile(turned_real, number // 2), tile(imag, number // 2)
                else:
                    ends = tile(real, number // 2), tile(turned_imag, number // 2)
                send[0, unit, block, shelf(chunk), :] = jnp.where(upper, *ends)

    pack(0)
    def launch(layer, unit):
        for place, plan in ((outer, PLANS[layer][unit % 2]), (inner, INNER[layer][unit % 2])):
            @pl.when(place)
            def _():
                for copy in copies(layer, unit, ranked(*plan)):
                    copy.start()

    def begin(groups):
        for group in groups:
            steps = [group * quarter + low for low in reversed(range(quarter))]
            for copy in copies(0, 0, [step for step in steps if step]):
                copy.start()

    pl.semaphore_wait(barrier, 2 * quarter - 1 + middle * quarter)

    @pl.when(inner)
    def _():
        greet(near_sem, 3 * quarter)
        greet(near_sem, quarter)
        begin((3,))

    begin((1, 0))
    for unit in range(1, units):
        pack(unit)
    pl.semaphore_wait(near_sem, 1)

    @pl.when(inner)
    def _():
        greet(far_sem, quarter)
        begin((2,))

    @pl.when(outer)
    def _():
        begin((2,))
        pl.semaphore_wait(far_sem, 1)
        begin((3,))

    for unit in range(units):
        recv[0, unit, me] = send[0, unit, me]
    norm_recv[me] = norm_send[...]

    moved = row_spin(True, True)
    next_bonds, sign_bonds = couplings([1, LAYERS])
    sine, cosine = sin_cos(field(moved, next_bonds, False))
    sine, cosine = spread(sine, True), spread(cosine, False)
    for unit in range(1, units):
        launch(0, unit)
    for copy in norms:
        copy.start()
    lanes = right_operand(rotation([turn(1, qubit) for qubit in range(LANE_BITS)], True))
    held = jnp.concatenate(
        split(
            rotation(
                [turn(1, LANE_BITS + bit) for bit in range(inner_bits)]
                + [None]
                + [turn(1, local_bits + bit) for bit in range(global_bits)]
            )
        ),
        axis=1,
    )
    late = [turn(1, LANE_BITS + inner_bits + bit) for bit in range(chunk_bits)]
    tops = [
        [turn(0, local_bits + bit) for bit in range(global_bits)],
        [turn(1, local_bits - global_bits + bit) for bit in range(global_bits)],
    ]
    energy_moved = spread(field(moved, sign_bonds, True), False)
    energy_plain = spread(field(row_spin(False, True), sign_bonds, True), False)

    def folded(parts, energy_field):
        total = jnp.zeros((TILE, LANES), F32)
        for chunk, values in enumerate(parts):
            weight = values * values * part(energy_field, chunk)
            for block in range(count):
                total = total + tile(weight, block)
        return jnp.sum(total, axis=0, keepdims=True)

    between = []
    for chunk in range(chunks):
        if chunk % depth == 0:
            blocks(0, chunk // depth).wait_recv()
        values = turn_blocks(received(0, chunk), tops[0])
        between.append(values)
        values = part(cosine, chunk) * values + part(sine, chunk) * flipped(values)
        values = apply_lanes(values, lanes)
        values = paired(held, right_operand(values))
        unit = chunk // depth
        send[1, unit, :, shelf(chunk), :] = values.reshape(count, TILE, LANES)
        if chunk % depth == depth - 1:
            launch(1, unit)
            recv[1, unit, me] = send[1, unit, me]

    energy_send[0:1] = folded(between, energy_moved)
    stats(0).wait_recv()
    amps_total = F32(2.0**qubits)
    norm = jnp.sum(jnp.sum(norm_recv[...], axis=0), axis=1, keepdims=True)
    factor = 1.0 / jnp.sqrt(norm / amps_total + 1e-06)
    phase = (held_ones + ones(small_row, inner_bits)) & 3
    even = (phase & 1) == 0
    sign = jnp.where((phase & 2) == 0, factor, -factor)
    along, across = jnp.where(even, sign, 0.0), jnp.where(even, 0.0, sign)
    frames = [
        (along, across * side),
        (-across, along * side),
        (-along, -across * side),
        (across, -along * side),
    ]

    parts = []
    for chunk in range(chunks):
        if chunk % depth == 0:
            blocks(1, chunk // depth).wait_recv()
        parts.append(turn_blocks(received(1, chunk), tops[1]))
        for bit, (cosine, sine) in enumerate(late):
            if (chunk + 1) % (2 << bit) == 0:
                for high in range(chunk + 1 - (1 << bit), chunk + 1):
                    low = high - (1 << bit)
                    parts[low], parts[high] = (
                        cosine * parts[low] - sine * parts[high],
                        cosine * parts[high] + sine * parts[low],
                    )

    energy_send[1:2] = folded(parts, energy_plain)
    for copy in weights:
        copy.start()
    energy_recv[me] = energy_send[...]
    for chunk, values in enumerate(parts):
        turned = flipped(values)
        for block in range(count):
            along, across = frames[(block.bit_count() + chunk.bit_count()) & 3]
            final = along * tile(values, block) + across * tile(turned, block)
            start = TILE * (block * chunks + chunk)
            out_ref[pl.ds(start, chunk_rows, 2), :] = final[:chunk_rows]
            out_ref[pl.ds(start + 1, chunk_rows, 2), :] = final[chunk_rows:]
    pltpu.make_async_remote_copy(
        src_ref=send.at[:, :, others],
        dst_ref=recv.at[:, :, others],
        send_sem=send_sem,
        recv_sem=recv_sems.at[0, 0],
        device_id={axis: peers[order[0]]},
        device_id_type=MESH,
    ).wait_send()
    stats(0).wait_send()
    stats(1).wait_recv()
    sums = jnp.sum(energy_recv[...], axis=0) * (factor * factor / amps_total)
    sums = jnp.sum(sums, axis=1, keepdims=True)
    which = lax.broadcasted_iota(jnp.int32, (1, LAYERS), 1)
    energy_ref[...] = jnp.where(which == 0, sums[0:1], sums[1:2])
    stats(1).wait_send()


def place(state_ref, energy_ref, state_out, energy_out, sems):
    moves = [
        pltpu.make_async_copy(state_ref, state_out, sems.at[0]),
        pltpu.make_async_copy(energy_ref, energy_out, sems.at[1]),
    ]
    for move in moves:
        move.start()
    for move in moves:
        move.wait()


def solution(mesh):
    axis = "amp"
    count = mesh.shape[axis]

    def local(amplitudes, coupling_index, rotation_index, chain_order, bond_sign):
        rows = amplitudes.shape[1] // LANES
        qubits = chain_order.shape[0]
        block_rows = rows // count
        chunk_rows = TILE // 2
        chunks = block_rows // chunk_rows
        depth = 2 if chunks % 2 == 0 else 1
        units = chunks // depth
        view = amplitudes.reshape(2, rows, LANES).transpose(1, 0, 2).reshape(2 * rows, LANES)
        vmem = pl.BlockSpec(memory_space=pltpu.VMEM)
        anywhere = pl.BlockSpec(memory_space=pl.ANY)
        state, energies = pl.pallas_call(
            functools.partial(kernel, axis, count, chunks, depth, qubits),
            out_shape=(
                pltpu.VMEM((2 * rows, LANES), F32),
                pltpu.VMEM((1, LAYERS), F32),
            ),
            in_specs=[anywhere] * 5,
            out_specs=(vmem, vmem),
            scratch_shapes=[
                pltpu.VMEM((2 * rows, LANES), F32),
                pltpu.SMEM(coupling_index.shape, jnp.int32),
                pltpu.SMEM(rotation_index.shape, jnp.int32),
                pltpu.SMEM(chain_order.shape, jnp.int32),
                pltpu.SMEM(bond_sign.shape, jnp.int32),
                pltpu.SMEM((2, ANGLES), F32),
                pltpu.VMEM((LAYERS, units, count, depth * TILE, LANES), F32),
                pltpu.VMEM((LAYERS, units, count, depth * TILE, LANES), F32),
                pltpu.VMEM((1, LANES), F32),
                pltpu.VMEM((count, 1, LANES), F32),
                pltpu.VMEM((LAYERS, LANES), F32),
                pltpu.VMEM((count, LAYERS, LANES), F32),
                pltpu.SemaphoreType.DMA((5,)),
                pltpu.SemaphoreType.DMA,
                pltpu.SemaphoreType.DMA((LAYERS, units)),
                pltpu.SemaphoreType.DMA((2,)),
                pltpu.SemaphoreType.DMA((2,)),
                pltpu.SemaphoreType.REGULAR,
                pltpu.SemaphoreType.REGULAR,
            ],
            compiler_params=pltpu.CompilerParams(collective_id=0, has_side_effects=True),
        )(view, coupling_index, rotation_index, chain_order, bond_sign)
        state, energies = pl.pallas_call(
            place,
            out_shape=(
                jax.ShapeDtypeStruct((2 * rows, LANES), F32),
                jax.ShapeDtypeStruct((1, LAYERS), F32),
            ),
            in_specs=[anywhere] * 2,
            out_specs=(anywhere, anywhere),
            scratch_shapes=[pltpu.SemaphoreType.DMA((2,))],
        )(*(pltpu.with_memory_space_constraint(x, pltpu.VMEM) for x in (state, energies)))
        state = state.reshape(rows, 2, LANES).transpose(1, 0, 2).reshape(2, rows * LANES)
        return state, energies.reshape(LAYERS)

    in_specs = (P(None, ("rep", "amp")), P("rep", None), P("rep", None), P(), P())
    out_specs = (P(None, ("rep", "amp")), P("rep"))
    return jax.shard_map(local, mesh=mesh, in_specs=in_specs, out_specs=out_specs, check_vma=False)
```

```python
import functools
import math

import jax
import jax.numpy as jnp
from jax import lax
from jax.experimental import pallas as pl
from jax.experimental.pallas import tpu as pltpu
from jax.sharding import PartitionSpec as P

LAYERS = 2
ANGLES = 16
LANES = 128
LANE_BITS = 7
TILE = 8
F32 = jnp.float32
BF16 = jnp.bfloat16
MESH = pl.DeviceIdType.MESH
DOWN = (3, 2, 1, 0)
PLANS = (
    (((2, 3, 1, 0), DOWN), ((1, 0, 2, 3), DOWN)),
    (((2, 1, 3, 0), DOWN), ((2, 3, 0, 1), DOWN)),
)
INNER = (
    (((2, 3, 1, 0), DOWN), ((1, 0, 2, 3), DOWN)),
    (((2, 3, 1, 0), DOWN), ((2, 3, 0, 1), DOWN)),
)


def angle(index):
    return (index + 1).astype(F32) * F32(math.pi / (2.0 * (ANGLES + 1)))


def mm(left, right):
    return jnp.dot(left, right, preferred_element_type=F32)


def split(values):
    high = values.astype(BF16)
    return high, (values - high.astype(F32)).astype(BF16)


def mm3(left, right):
    return mm(left[0], right[0]) + mm(left[1], right[0]) + mm(left[0], right[1])


def mm_exact_left(left, values):
    high = values.astype(BF16)
    rest = values - high.astype(F32)
    middle = rest.astype(BF16)
    low = (rest - middle.astype(F32)).astype(BF16)
    return mm(left, high) + mm(left, middle) + mm(left, low)


def mm_exact_right(values, right):
    high = values.astype(BF16)
    rest = values - high.astype(F32)
    middle = rest.astype(BF16)
    low = (rest - middle.astype(F32)).astype(BF16)
    joined = jnp.concatenate([high, middle], axis=1)
    return mm(joined, jnp.concatenate([right, right], axis=0)) + mm(low, right)


def sin_cos(values):
    turns = jnp.floor(values * F32(1.0 / math.pi) + 0.5)
    rest = values - turns * F32(3.140625)
    rest = rest - turns * F32(9.67502593994140625e-4)
    rest = rest - turns * F32(1.509957990978376432e-7)
    sign = 1.0 - 2.0 * (turns - 2.0 * jnp.floor(turns * 0.5))
    square = rest * rest
    sine = F32(-1.0 / 39916800)
    for coefficient in (1.0 / 362880, -1.0 / 5040, 1.0 / 120, -1.0 / 6, 1.0):
        sine = sine * square + F32(coefficient)
    cosine = F32(-1.0 / 3628800)
    for coefficient in (1.0 / 40320, -1.0 / 720, 1.0 / 24, -0.5, 1.0):
        cosine = cosine * square + F32(coefficient)
    return sine * (rest * sign), cosine * sign


def rotation(pairs, transposed=False):
    base = min(len(pairs), LANE_BITS)
    shape = (TILE, 2**base)
    row = lax.broadcasted_iota(jnp.int32, shape, 0)
    column = lax.broadcasted_iota(jnp.int32, shape, 1)

    def factors(bit):
        pair = pairs[bit]
        cosine, sine = (F32(1.0), F32(0.0)) if pair is None else pair
        if transposed:
            sine = -sine
        here = ((column >> bit) & 1) == 1
        return jnp.where(here, -sine, cosine), jnp.where(here, cosine, sine)

    value = None
    for bit in range(3):
        clear, put = factors(bit)
        factor = jnp.where(((row >> bit) & 1) == 1, put, clear)
        value = factor if value is None else value * factor
    found = [value]
    for bit in range(3, base):
        clear, put = factors(bit)
        found = [value * clear for value in found] + [value * put for value in found]
    value = jnp.concatenate(found, axis=0)
    for cosine, sine in pairs[base:]:
        value = jnp.concatenate(
            [
                jnp.concatenate([cosine * value, -sine * value], axis=1),
                jnp.concatenate([sine * value, cosine * value], axis=1),
            ],
            axis=0,
        )
    return value


def right_operand(matrix):
    high, low = split(matrix)
    return jnp.concatenate(
        [
            jnp.concatenate([high, low], axis=1),
            jnp.concatenate([high, jnp.zeros_like(high)], axis=1),
        ],
        axis=0,
    )


def paired(left, right):
    both = mm(left, right)
    return both[:, :LANES] + both[:, LANES:]


def apply_lanes(values, operand):
    return paired(jnp.concatenate(split(values), axis=1), operand)


def turn_blocks(values, pairs):
    height = values.shape[0]
    for bit, (cosine, sine) in enumerate(pairs):
        width = TILE << bit
        parts = []
        for start in range(0, height, 2 * width):
            low = values[start : start + width]
            high = values[start + width : start + 2 * width]
            parts += [cosine * low - sine * high, cosine * high + sine * low]
        values = jnp.concatenate(parts, axis=0)
    return values


def flipped(values):
    groups = values.reshape(values.shape[0] // TILE, TILE, LANES)
    return pltpu.roll(groups, TILE // 2, 1).reshape(values.shape)


def kernel(
    axis, count, chunks, depth, qubits,
    state_hbm, couple_hbm, turn_hbm, order_hbm, sign_hbm,
    out_ref, energy_ref,
    state_ref, couple_ref, turn_ref, order_ref, sign_ref,
    table, send, recv, norm_send, norm_recv, energy_send, energy_recv,
    local_sems, send_sem, recv_sems, stat_send_sems, stat_recv_sems, near_sem, far_sem,
):
    me = lax.axis_index(axis)
    rows = state_ref.shape[0] // 2
    row_bits = rows.bit_length() - 1
    global_bits = count.bit_length() - 1
    local_bits = row_bits + LANE_BITS
    block_rows = rows // count
    low_bits = row_bits - global_bits
    chunk_bits = chunks.bit_length() - 1
    chunk_rows = block_rows // chunks
    inner_bits = low_bits - chunk_bits
    tiles = rows // chunk_rows
    units = chunks // depth
    def ranked(groups, inner):
        size = count // 4
        steps = [
            group * size + high * (size // 4) + low
            for group in groups
            for high in inner
            for low in range(size // 4)
        ]
        return [step for step in steps if step]

    order = ranked((2, 3, 1, 0), (3, 2, 1, 0))
    flips = [(1 - 2 * lax.rem(me // 2**bit, 2)) * 2**bit for bit in range(global_bits)]
    peers = {
        step: me + sum(flips[bit] for bit in range(global_bits) if step >> bit & 1)
        for step in order
    }

    quarter = count // 4
    top, second_bit = lax.div(me, 2 * quarter), lax.rem(lax.div(me, quarter), 2)
    middle = top + second_bit - 2 * top * second_bit
    inner = middle == 1
    outer = middle == 0

    def greet(semaphore, step):
        pl.semaphore_signal(
            semaphore, inc=1, device_id={axis: peers[step]}, device_id_type=MESH
        )

    barrier = pltpu.get_barrier_semaphore()

    @pl.when(inner)
    def _():
        for step in range(3 * quarter, count):
            greet(barrier, step)

    for step in range(2 * quarter - 1, 0, -1):
        greet(barrier, step)
    arrivals = [
        pltpu.make_async_copy(source, target, local_sems.at[number])
        for number, (source, target) in enumerate(
            [
                (couple_hbm, couple_ref),
                (turn_hbm, turn_ref),
                (order_hbm, order_ref),
                (sign_hbm, sign_ref),
                (state_hbm, state_ref),
            ]
        )
    ]
    for copy in arrivals:
        copy.start()


    for entry in range(ANGLES):
        theta = (entry + 1) * math.pi / (2.0 * (ANGLES + 1))
        table[0, entry] = F32(math.cos(theta))
        table[1, entry] = F32(math.sin(theta))
    for copy in arrivals[:-1]:
        copy.wait()

    def turn(layer, qubit):
        index = turn_ref[layer, qubit]
        return table[0, index], table[1, index]

    height = -(-qubits // 8) * 8
    place = lax.broadcasted_iota(jnp.int32, (height, LANES), 0) * LANES + (
        lax.broadcasted_iota(jnp.int32, (height, LANES), 1)
    )

    def couplings(layers):
        matrices = [jnp.zeros((height, LANES), F32) for _ in layers]
        for bond in range(qubits - 1):
            start, end = order_ref[bond], order_ref[bond + 1]
            here = (place == start * LANES + end) | (place == end * LANES + start)
            for number, layer in enumerate(layers):
                value = (2 * sign_ref[bond] - 1).astype(F32)
                if layer < LAYERS:
                    value = angle(couple_ref[layer, bond]) * value
                matrices[number] = jnp.where(here, value, matrices[number])
        rest = jnp.zeros((LANES - height, LANES), F32)
        return [jnp.concatenate([matrix, rest], axis=0) for matrix in matrices]

    square_row = lax.broadcasted_iota(jnp.int32, (LANES, LANES), 0)
    square_lane = lax.broadcasted_iota(jnp.int32, (LANES, LANES), 1)
    lane_spin = (1 - 2 * ((square_lane >> jnp.minimum(square_row, 31)) & 1)).astype(F32)
    lane_only = jnp.where(square_row < LANE_BITS, lane_spin, 0.0)
    lane_ones = jnp.where(square_row < LANE_BITS, lane_spin, 1.0).astype(BF16)
    row_index = lax.broadcasted_iota(jnp.int32, (rows, LANES), 0)
    lane_index = lax.broadcasted_iota(jnp.int32, (rows, LANES), 1)

    def row_spin(swapped, chunked):
        held = row_index
        if chunked:
            inner = held & (chunk_rows - 1)
            block = (held >> inner_bits) & (count - 1)
            chunk = held >> (inner_bits + global_bits)
            held = inner + (chunk << inner_bits) + (block << low_bits)
        if swapped:
            low, high = held & (block_rows - 1), held >> low_bits
            index = low + (me << low_bits) + (high << row_bits)
        else:
            index = held + (me << row_bits)
        spin = (1 - 2 * ((index >> jnp.clip(lane_index - LANE_BITS, 0, 31)) & 1)).astype(F32)
        return jnp.where((lane_index >= LANE_BITS) & (lane_index < qubits), spin, 0.0)

    def field(spin, matrix, exact, half=None):
        if half is not None:
            pass
        elif exact:
            half = mm(spin.astype(BF16), matrix.astype(BF16))
        else:
            half = mm_exact_left(spin.astype(BF16), matrix)
        half = jnp.where(lane_index < LANE_BITS, half, 0.5 * half * spin)
        lane_pairs = 0.5 * jnp.sum(
            mm_exact_right(matrix[:TILE], lane_only.astype(BF16)) * lane_only[:TILE],
            axis=0,
            keepdims=True,
        )
        if exact:
            return mm(half.astype(BF16), lane_ones) + lane_pairs
        return mm_exact_right(half, lane_ones) + lane_pairs

    def copies(layer, unit, steps):
        return [
            pltpu.make_async_remote_copy(
                src_ref=send.at[layer, unit, peers[step]],
                dst_ref=recv.at[layer, unit, me],
                send_sem=send_sem,
                recv_sem=recv_sems.at[layer, unit],
                device_id={axis: peers[step]},
                device_id_type=MESH,
            )
            for step in steps
        ]

    def stat_copies(which):
        return [
            pltpu.make_async_remote_copy(
                src_ref=(norm_send, energy_send)[which],
                dst_ref=(norm_recv, energy_recv)[which].at[me],
                send_sem=stat_send_sems.at[which],
                recv_sem=stat_recv_sems.at[which],
                device_id={axis: peers[step]},
                device_id_type=MESH,
            )
            for step in order
        ]

    others = pl.ds(0, count - 1)

    def blocks(layer, unit):
        return pltpu.make_async_remote_copy(
            src_ref=send.at[layer, unit, others],
            dst_ref=recv.at[layer, unit, others],
            send_sem=send_sem,
            recv_sem=recv_sems.at[layer, unit],
            device_id={axis: peers[order[0]]},
            device_id_type=MESH,
        )

    def shelf(chunk):
        start = chunk % depth * TILE
        return slice(start, start + TILE)

    def received(layer, chunk):
        values = recv[layer, chunk // depth, :, shelf(chunk), :]
        return values.reshape(count * TILE, LANES)

    def stats(which):
        return pltpu.make_async_remote_copy(
            src_ref=(norm_recv, energy_recv)[which].at[others],
            dst_ref=(norm_recv, energy_recv)[which].at[others],
            send_sem=stat_send_sems.at[which],
            recv_sem=stat_recv_sems.at[which],
            device_id={axis: peers[order[0]]},
            device_id_type=MESH,
        )

    upper = lax.broadcasted_iota(jnp.int32, (TILE, LANES), 0) < TILE // 2
    side = jnp.where(upper, F32(1.0), F32(-1.0))

    def tile(values, number):
        return values[number * TILE : (number + 1) * TILE]

    def spread(values, signed):
        turned = flipped(values)
        found = []
        for number in range(tiles):
            here, there = tile(values, number // 2), tile(turned, number // 2)
            if number % 2:
                here, there = there, here
            both = jnp.where(upper, here, there)
            found.append(both * side if signed else both)
        return found

    def part(found, chunk):
        return jnp.concatenate(found[chunk * count : (chunk + 1) * count], axis=0)

    def ones(values, bits):
        return sum((values >> bit) & 1 for bit in range(bits))

    small_row = lax.broadcasted_iota(jnp.int32, (TILE, LANES), 0)
    small_lane = lax.broadcasted_iota(jnp.int32, (TILE, LANES), 1)
    held_ones = ones(small_lane, LANE_BITS) + sum(
        lax.rem(lax.div(me, 2**bit), 2) for bit in range(global_bits)
    )
    quarters = [
        ((held_ones + ones(small_row, 3) + more) & 3).astype(F32) * F32(-math.pi / 2)
        for more in range(4)
    ]
    frame = jnp.concatenate(
        [quarters[number.bit_count() & 3] for number in range(rows // TILE)], axis=0
    )

    def doubled(first, step):
        found = [first]
        for bit in range(3, row_bits):
            found = sum(zip(*[step(value, bit) for value in found]), ())
        return jnp.concatenate(found, axis=0)

    def own_spin(bit):
        if bit < row_bits:
            return (1 - 2 * ((small_row >> bit) & 1)).astype(F32)
        bit = bit - row_bits
        return (1 - 2 * lax.rem(lax.div(me, 2**bit), 2)).astype(F32)

    own_bits = list(range(3)) + list(range(row_bits, row_bits + global_bits))
    above = small_lane - LANE_BITS
    first_spin = jnp.where((above >= 0) & (above < row_bits), F32(1.0), F32(0.0))
    for bit in own_bits:
        first_spin = jnp.where(above == bit, own_spin(bit), first_spin)
    bonds = couplings([0])[0]

    def bond_row(bit):
        return bonds[LANE_BITS + bit : LANE_BITS + bit + 1]

    spin = doubled(
        first_spin,
        lambda value, bit: (value, jnp.where(above == bit, -value, value)),
    )
    half = doubled(
        sum(own_spin(bit) * bond_row(bit) for bit in own_bits),
        lambda value, bit: (value + bond_row(bit), value - bond_row(bit)),
    )
    sine, cosine = sin_cos(field(spin, bonds, False, half) + frame)
    lanes = right_operand(rotation([turn(0, qubit) for qubit in range(LANE_BITS)], True))
    held = split(rotation([turn(0, LANE_BITS + bit) for bit in range(row_bits)]))

    arrivals[-1].wait()
    real = state_ref[pl.ds(0, rows, 2), :]
    imag = state_ref[pl.ds(1, rows, 2), :]
    norm_send[...] = jnp.sum(real * real + imag * imag, axis=0, keepdims=True)
    real, imag = cosine * real + sine * imag, cosine * imag - sine * real
    both = apply_lanes(jnp.concatenate([real, imag], axis=0), lanes)
    both = mm3(held, split(jnp.concatenate([both[:rows], both[rows:]], axis=1)))
    real, imag = both[:, :LANES], both[:, LANES:]
    turned_real, turned_imag = flipped(real), flipped(imag)
    norms, weights = stat_copies(0), stat_copies(1)
    def pack(unit):
        for chunk in range(unit * depth, unit * depth + depth):
            for block in range(count):
                number = block * chunks + chunk
                if number % 2:
                    ends = tile(turned_real, number // 2), tile(imag, number // 2)
                else:
                    ends = tile(real, number // 2), tile(turned_imag, number // 2)
                send[0, unit, block, shelf(chunk), :] = jnp.where(upper, *ends)

    pack(0)
    def launch(layer, unit):
        for place, plan in ((outer, PLANS[layer][unit % 2]), (inner, INNER[layer][unit % 2])):
            @pl.when(place)
            def _():
                for copy in copies(layer, unit, ranked(*plan)):
                    copy.start()

    def begin(groups):
        for group in groups:
            steps = [group * quarter + low for low in reversed(range(quarter))]
            for copy in copies(0, 0, [step for step in steps if step]):
                copy.start()

    pl.semaphore_wait(barrier, 2 * quarter - 1 + middle * quarter)

    @pl.when(inner)
    def _():
        greet(near_sem, 3 * quarter)
        greet(near_sem, quarter)
        begin((3,))

    begin((1, 0))
    for unit in range(1, units):
        pack(unit)
    pl.semaphore_wait(near_sem, 1)

    @pl.when(inner)
    def _():
        greet(far_sem, quarter)
        begin((2,))

    @pl.when(outer)
    def _():
        begin((2,))
        pl.semaphore_wait(far_sem, 1)
        begin((3,))

    for unit in range(units):
        recv[0, unit, me] = send[0, unit, me]
    norm_recv[me] = norm_send[...]

    moved = row_spin(True, True)
    next_bonds, sign_bonds = couplings([1, LAYERS])
    sine, cosine = sin_cos(field(moved, next_bonds, False))
    sine, cosine = spread(sine, True), spread(cosine, False)
    for unit in range(1, units):
        launch(0, unit)
    for copy in norms:
        copy.start()
    lanes = right_operand(rotation([turn(1, qubit) for qubit in range(LANE_BITS)], True))
    held = jnp.concatenate(
        split(
            rotation(
                [turn(1, LANE_BITS + bit) for bit in range(inner_bits)]
                + [None]
                + [turn(1, local_bits + bit) for bit in range(global_bits)]
            )
        ),
        axis=1,
    )
    late = [turn(1, LANE_BITS + inner_bits + bit) for bit in range(chunk_bits)]
    tops = [
        [turn(0, local_bits + bit) for bit in range(global_bits)],
        [turn(1, local_bits - global_bits + bit) for bit in range(global_bits)],
    ]
    energy_moved = spread(field(moved, sign_bonds, True), False)
    energy_plain = spread(field(row_spin(False, True), sign_bonds, True), False)

    def folded(parts, energy_field):
        total = jnp.zeros((TILE, LANES), F32)
        for chunk, values in enumerate(parts):
            weight = values * values * part(energy_field, chunk)
            for block in range(count):
                total = total + tile(weight, block)
        return jnp.sum(total, axis=0, keepdims=True)

    between = []
    for chunk in range(chunks):
        if chunk % depth == 0:
            blocks(0, chunk // depth).wait_recv()
        values = turn_blocks(received(0, chunk), tops[0])
        between.append(values)
        values = part(cosine, chunk) * values + part(sine, chunk) * flipped(values)
        values = apply_lanes(values, lanes)
        values = paired(held, right_operand(values))
        unit = chunk // depth
        send[1, unit, :, shelf(chunk), :] = values.reshape(count, TILE, LANES)
        if chunk % depth == depth - 1:
            launch(1, unit)
            recv[1, unit, me] = send[1, unit, me]

    energy_send[0:1] = folded(between, energy_moved)
    stats(0).wait_recv()
    amps_total = F32(2.0**qubits)
    norm = jnp.sum(jnp.sum(norm_recv[...], axis=0), axis=1, keepdims=True)
    factor = 1.0 / jnp.sqrt(norm / amps_total + 1e-06)
    phase = (held_ones + ones(small_row, inner_bits)) & 3
    even = (phase & 1) == 0
    sign = jnp.where((phase & 2) == 0, factor, -factor)
    along, across = jnp.where(even, sign, 0.0), jnp.where(even, 0.0, sign)
    frames = [
        (along, across * side),
        (-across, along * side),
        (-along, -across * side),
        (across, -along * side),
    ]

    parts = []
    for chunk in range(chunks):
        if chunk % depth == 0:
            blocks(1, chunk // depth).wait_recv()
        parts.append(turn_blocks(received(1, chunk), tops[1]))
        for bit, (cosine, sine) in enumerate(late):
            if (chunk + 1) % (2 << bit) == 0:
                for high in range(chunk + 1 - (1 << bit), chunk + 1):
                    low = high - (1 << bit)
                    parts[low], parts[high] = (
                        cosine * parts[low] - sine * parts[high],
                        cosine * parts[high] + sine * parts[low],
                    )

    energy_send[1:2] = folded(parts, energy_plain)
    for copy in weights:
        copy.start()
    energy_recv[me] = energy_send[...]
    for chunk, values in enumerate(parts):
        turned = flipped(values)
        for block in range(count):
            along, across = frames[(block.bit_count() + chunk.bit_count()) & 3]
            final = along * tile(values, block) + across * tile(turned, block)
            start = TILE * (block * chunks + chunk)
            out_ref[pl.ds(start, chunk_rows, 2), :] = final[:chunk_rows]
            out_ref[pl.ds(start + 1, chunk_rows, 2), :] = final[chunk_rows:]
    pltpu.make_async_remote_copy(
        src_ref=send.at[:, :, others],
        dst_ref=recv.at[:, :, others],
        send_sem=send_sem,
        recv_sem=recv_sems.at[0, 0],
        device_id={axis: peers[order[0]]},
        device_id_type=MESH,
    ).wait_send()
    stats(0).wait_send()
    stats(1).wait_recv()
    sums = jnp.sum(energy_recv[...], axis=0) * (factor * factor / amps_total)
    sums = jnp.sum(sums, axis=1, keepdims=True)
    which = lax.broadcasted_iota(jnp.int32, (1, LAYERS), 1)
    energy_ref[...] = jnp.where(which == 0, sums[0:1], sums[1:2])
    stats(1).wait_send()


def place(state_ref, energy_ref, state_out, energy_out, sems):
    moves = [
        pltpu.make_async_copy(state_ref, state_out, sems.at[0]),
        pltpu.make_async_copy(energy_ref, energy_out, sems.at[1]),
    ]
    for move in moves:
        move.start()
    for move in moves:
        move.wait()


def solution(mesh):
    axis = "amp"
    count = mesh.shape[axis]

    def local(amplitudes, coupling_index, rotation_index, chain_order, bond_sign):
        rows = amplitudes.shape[1] // LANES
        qubits = chain_order.shape[0]
        block_rows = rows // count
        chunk_rows = TILE // 2
        chunks = block_rows // chunk_rows
        depth = 2 if chunks % 2 == 0 else 1
        units = chunks // depth
        view = amplitudes.reshape(2, rows, LANES).transpose(1, 0, 2).reshape(2 * rows, LANES)
        vmem = pl.BlockSpec(memory_space=pltpu.VMEM)
        anywhere = pl.BlockSpec(memory_space=pl.ANY)
        state, energies = pl.pallas_call(
            functools.partial(kernel, axis, count, chunks, depth, qubits),
            out_shape=(
                pltpu.VMEM((2 * rows, LANES), F32),
                pltpu.VMEM((1, LAYERS), F32),
            ),
            in_specs=[anywhere] * 5,
            out_specs=(vmem, vmem),
            scratch_shapes=[
                pltpu.VMEM((2 * rows, LANES), F32),
                pltpu.SMEM(coupling_index.shape, jnp.int32),
                pltpu.SMEM(rotation_index.shape, jnp.int32),
                pltpu.SMEM(chain_order.shape, jnp.int32),
                pltpu.SMEM(bond_sign.shape, jnp.int32),
                pltpu.SMEM((2, ANGLES), F32),
                pltpu.VMEM((LAYERS, units, count, depth * TILE, LANES), F32),
                pltpu.VMEM((LAYERS, units, count, depth * TILE, LANES), F32),
                pltpu.VMEM((1, LANES), F32),
                pltpu.VMEM((count, 1, LANES), F32),
                pltpu.VMEM((LAYERS, LANES), F32),
                pltpu.VMEM((count, LAYERS, LANES), F32),
                pltpu.SemaphoreType.DMA((5,)),
                pltpu.SemaphoreType.DMA,
                pltpu.SemaphoreType.DMA((LAYERS, units)),
                pltpu.SemaphoreType.DMA((2,)),
                pltpu.SemaphoreType.DMA((2,)),
                pltpu.SemaphoreType.REGULAR,
                pltpu.SemaphoreType.REGULAR,
            ],
            compiler_params=pltpu.CompilerParams(collective_id=0, has_side_effects=True),
        )(view, coupling_index, rotation_index, chain_order, bond_sign)
        state, energies = pl.pallas_call(
            place,
            out_shape=(
                jax.ShapeDtypeStruct((2 * rows, LANES), F32),
                jax.ShapeDtypeStruct((1, LAYERS), F32),
            ),
            in_specs=[anywhere] * 2,
            out_specs=(anywhere, anywhere),
            scratch_shapes=[pltpu.SemaphoreType.DMA((2,))],
        )(*(pltpu.with_memory_space_constraint(x, pltpu.VMEM) for x in (state, energies)))
        state = state.reshape(rows, 2, LANES).transpose(1, 0, 2).reshape(2, rows * LANES)
        return state, energies.reshape(LAYERS)

    in_specs = (P(None, ("rep", "amp")), P("rep", None), P("rep", None), P(), P())
    out_specs = (P(None, ("rep", "amp")), P("rep"))
    return jax.shard_map(local, mesh=mesh, in_specs=in_specs, out_specs=out_specs, check_vma=False)
```

```python
import functools
import math

import jax
import jax.numpy as jnp
from jax import lax
from jax.experimental import pallas as pl
from jax.experimental.pallas import tpu as pltpu
from jax.sharding import PartitionSpec as P

LAYERS = 2
ANGLES = 16
LANES = 128
LANE_BITS = 7
TILE = 8
F32 = jnp.float32
BF16 = jnp.bfloat16
MESH = pl.DeviceIdType.MESH
DOWN = (3, 2, 1, 0)
PLANS = (
    (((2, 3, 1, 0), DOWN), ((1, 0, 2, 3), DOWN)),
    (((2, 1, 3, 0), DOWN), ((2, 3, 0, 1), DOWN)),
)
INNER = (
    (((2, 3, 1, 0), DOWN), ((1, 0, 2, 3), DOWN)),
    (((2, 3, 1, 0), DOWN), ((2, 3, 0, 1), DOWN)),
)


def angle(index):
    return (index + 1).astype(F32) * F32(math.pi / (2.0 * (ANGLES + 1)))


def mm(left, right):
    return jnp.dot(left, right, preferred_element_type=F32)


def split(values):
    high = values.astype(BF16)
    return high, (values - high.astype(F32)).astype(BF16)


def mm3(left, right):
    return mm(left[0], right[0]) + mm(left[1], right[0]) + mm(left[0], right[1])


def mm_exact_left(left, values):
    high = values.astype(BF16)
    rest = values - high.astype(F32)
    middle = rest.astype(BF16)
    low = (rest - middle.astype(F32)).astype(BF16)
    return mm(left, high) + mm(left, middle) + mm(left, low)


def mm_exact_right(values, right):
    high = values.astype(BF16)
    rest = values - high.astype(F32)
    middle = rest.astype(BF16)
    low = (rest - middle.astype(F32)).astype(BF16)
    return mm(high, right) + mm(middle, right) + mm(low, right)


def sin_cos(values):
    turns = jnp.floor(values * F32(1.0 / math.pi) + 0.5)
    rest = values - turns * F32(3.140625)
    rest = rest - turns * F32(9.67502593994140625e-4)
    rest = rest - turns * F32(1.509957990978376432e-7)
    sign = 1.0 - 2.0 * (turns - 2.0 * jnp.floor(turns * 0.5))
    square = rest * rest
    sine = F32(-1.0 / 39916800)
    for coefficient in (1.0 / 362880, -1.0 / 5040, 1.0 / 120, -1.0 / 6, 1.0):
        sine = sine * square + F32(coefficient)
    cosine = F32(-1.0 / 3628800)
    for coefficient in (1.0 / 40320, -1.0 / 720, 1.0 / 24, -0.5, 1.0):
        cosine = cosine * square + F32(coefficient)
    return sine * (rest * sign), cosine * sign


def rotation(pairs, transposed=False):
    base = min(len(pairs), LANE_BITS)
    shape = (TILE, 2**base)
    row = lax.broadcasted_iota(jnp.int32, shape, 0)
    column = lax.broadcasted_iota(jnp.int32, shape, 1)

    def factors(bit):
        pair = pairs[bit]
        cosine, sine = (F32(1.0), F32(0.0)) if pair is None else pair
        if transposed:
            sine = -sine
        here = ((column >> bit) & 1) == 1
        return jnp.where(here, -sine, cosine), jnp.where(here, cosine, sine)

    value = None
    for bit in range(3):
        clear, put = factors(bit)
        factor = jnp.where(((row >> bit) & 1) == 1, put, clear)
        value = factor if value is None else value * factor
    found = [value]
    for bit in range(3, base):
        clear, put = factors(bit)
        found = [value * clear for value in found] + [value * put for value in found]
    value = jnp.concatenate(found, axis=0)
    for cosine, sine in pairs[base:]:
        value = jnp.concatenate(
            [
                jnp.concatenate([cosine * value, -sine * value], axis=1),
                jnp.concatenate([sine * value, cosine * value], axis=1),
            ],
            axis=0,
        )
    return value


def right_operand(matrix):
    high, low = split(matrix)
    return jnp.concatenate(
        [
            jnp.concatenate([high, low], axis=1),
            jnp.concatenate([high, jnp.zeros_like(high)], axis=1),
        ],
        axis=0,
    )


def paired(left, right):
    both = mm(left, right)
    return both[:, :LANES] + both[:, LANES:]


def apply_lanes(values, operand):
    return paired(jnp.concatenate(split(values), axis=1), operand)


def turn_blocks(values, pairs):
    height = values.shape[0]
    for bit, (cosine, sine) in enumerate(pairs):
        width = TILE << bit
        parts = []
        for start in range(0, height, 2 * width):
            low = values[start : start + width]
            high = values[start + width : start + 2 * width]
            parts += [cosine * low - sine * high, cosine * high + sine * low]
        values = jnp.concatenate(parts, axis=0)
    return values


def flipped(values):
    groups = values.reshape(values.shape[0] // TILE, TILE, LANES)
    return pltpu.roll(groups, TILE // 2, 1).reshape(values.shape)


def kernel(
    axis, count, chunks, depth, qubits,
    state_hbm, couple_hbm, turn_hbm, order_hbm, sign_hbm,
    out_ref, energy_ref,
    state_ref, couple_ref, turn_ref, order_ref, sign_ref,
    table, send, recv, norm_send, norm_recv, energy_send, energy_recv,
    local_sems, send_sem, recv_sems, stat_send_sems, stat_recv_sems, near_sem, far_sem,
):
    me = lax.axis_index(axis)
    rows = state_ref.shape[0] // 2
    row_bits = rows.bit_length() - 1
    global_bits = count.bit_length() - 1
    local_bits = row_bits + LANE_BITS
    block_rows = rows // count
    low_bits = row_bits - global_bits
    chunk_bits = chunks.bit_length() - 1
    chunk_rows = block_rows // chunks
    inner_bits = low_bits - chunk_bits
    tiles = rows // chunk_rows
    units = chunks // depth
    def ranked(groups, inner):
        size = count // 4
        steps = [
            group * size + high * (size // 4) + low
            for group in groups
            for high in inner
            for low in range(size // 4)
        ]
        return [step for step in steps if step]

    order = ranked((2, 3, 1, 0), (3, 2, 1, 0))
    flips = [(1 - 2 * lax.rem(me // 2**bit, 2)) * 2**bit for bit in range(global_bits)]
    peers = {
        step: me + sum(flips[bit] for bit in range(global_bits) if step >> bit & 1)
        for step in order
    }

    quarter = count // 4
    top, second_bit = lax.div(me, 2 * quarter), lax.rem(lax.div(me, quarter), 2)
    middle = top + second_bit - 2 * top * second_bit
    inner = middle == 1
    outer = middle == 0

    def greet(semaphore, step):
        pl.semaphore_signal(
            semaphore, inc=1, device_id={axis: peers[step]}, device_id_type=MESH
        )

    barrier = pltpu.get_barrier_semaphore()

    arrivals = [
        pltpu.make_async_copy(source, target, local_sems.at[number])
        for number, (source, target) in enumerate(
            [
                (couple_hbm, couple_ref),
                (turn_hbm, turn_ref),
                (order_hbm, order_ref),
                (sign_hbm, sign_ref),
                (state_hbm, state_ref),
            ]
        )
    ]
    for copy in arrivals:
        copy.start()

    @pl.when(inner)
    def _():
        for step in range(3 * quarter, count):
            greet(barrier, step)

    for step in range(2 * quarter - 1, 0, -1):
        greet(barrier, step)


    for entry in range(ANGLES):
        theta = (entry + 1) * math.pi / (2.0 * (ANGLES + 1))
        table[0, entry] = F32(math.cos(theta))
        table[1, entry] = F32(math.sin(theta))
    for copy in arrivals[:-1]:
        copy.wait()

    def turn(layer, qubit):
        index = turn_ref[layer, qubit]
        return table[0, index], table[1, index]

    height = -(-qubits // 8) * 8
    place = lax.broadcasted_iota(jnp.int32, (height, LANES), 0) * LANES + (
        lax.broadcasted_iota(jnp.int32, (height, LANES), 1)
    )

    def couplings(layers):
        matrices = [jnp.zeros((height, LANES), F32) for _ in layers]
        for bond in range(qubits - 1):
            start, end = order_ref[bond], order_ref[bond + 1]
            here = (place == start * LANES + end) | (place == end * LANES + start)
            for number, layer in enumerate(layers):
                value = (2 * sign_ref[bond] - 1).astype(F32)
                if layer < LAYERS:
                    value = angle(couple_ref[layer, bond]) * value
                matrices[number] = jnp.where(here, value, matrices[number])
        rest = jnp.zeros((LANES - height, LANES), F32)
        return [jnp.concatenate([matrix, rest], axis=0) for matrix in matrices]

    square_row = lax.broadcasted_iota(jnp.int32, (LANES, LANES), 0)
    square_lane = lax.broadcasted_iota(jnp.int32, (LANES, LANES), 1)
    lane_spin = (1 - 2 * ((square_lane >> jnp.minimum(square_row, 31)) & 1)).astype(F32)
    lane_only = jnp.where(square_row < LANE_BITS, lane_spin, 0.0)
    lane_ones = jnp.where(square_row < LANE_BITS, lane_spin, 1.0).astype(BF16)
    row_index = lax.broadcasted_iota(jnp.int32, (rows, LANES), 0)
    lane_index = lax.broadcasted_iota(jnp.int32, (rows, LANES), 1)

    def row_spin(swapped, chunked):
        held = row_index
        if chunked:
            inner = held & (chunk_rows - 1)
            block = (held >> inner_bits) & (count - 1)
            chunk = held >> (inner_bits + global_bits)
            held = inner + (chunk << inner_bits) + (block << low_bits)
        if swapped:
            low, high = held & (block_rows - 1), held >> low_bits
            index = low + (me << low_bits) + (high << row_bits)
        else:
            index = held + (me << row_bits)
        spin = (1 - 2 * ((index >> jnp.clip(lane_index - LANE_BITS, 0, 31)) & 1)).astype(F32)
        return jnp.where((lane_index >= LANE_BITS) & (lane_index < qubits), spin, 0.0)

    def field(spin, matrix, exact, half=None):
        if half is not None:
            pass
        elif exact:
            half = mm(spin.astype(BF16), matrix.astype(BF16))
        else:
            half = mm_exact_left(spin.astype(BF16), matrix)
        half = jnp.where(lane_index < LANE_BITS, half, 0.5 * half * spin)
        lane_pairs = 0.5 * jnp.sum(
            mm_exact_right(matrix[:TILE], lane_only.astype(BF16)) * lane_only[:TILE],
            axis=0,
            keepdims=True,
        )
        if exact:
            return mm(half.astype(BF16), lane_ones) + lane_pairs
        return mm_exact_right(half, lane_ones) + lane_pairs

    def copies(layer, unit, steps):
        return [
            pltpu.make_async_remote_copy(
                src_ref=send.at[layer, unit, peers[step]],
                dst_ref=recv.at[layer, unit, me],
                send_sem=send_sem,
                recv_sem=recv_sems.at[layer, unit],
                device_id={axis: peers[step]},
                device_id_type=MESH,
            )
            for step in steps
        ]

    def stat_copies(which):
        return [
            pltpu.make_async_remote_copy(
                src_ref=(norm_send, energy_send)[which],
                dst_ref=(norm_recv, energy_recv)[which].at[me],
                send_sem=stat_send_sems.at[which],
                recv_sem=stat_recv_sems.at[which],
                device_id={axis: peers[step]},
                device_id_type=MESH,
            )
            for step in order
        ]

    others = pl.ds(0, count - 1)

    def blocks(layer, unit):
        return pltpu.make_async_remote_copy(
            src_ref=send.at[layer, unit, others],
            dst_ref=recv.at[layer, unit, others],
            send_sem=send_sem,
            recv_sem=recv_sems.at[layer, unit],
            device_id={axis: peers[order[0]]},
            device_id_type=MESH,
        )

    def shelf(chunk):
        start = chunk % depth * TILE
        return slice(start, start + TILE)

    def received(layer, chunk):
        values = recv[layer, chunk // depth, :, shelf(chunk), :]
        return values.reshape(count * TILE, LANES)

    def stats(which):
        return pltpu.make_async_remote_copy(
            src_ref=(norm_recv, energy_recv)[which].at[others],
            dst_ref=(norm_recv, energy_recv)[which].at[others],
            send_sem=stat_send_sems.at[which],
            recv_sem=stat_recv_sems.at[which],
            device_id={axis: peers[order[0]]},
            device_id_type=MESH,
        )

    upper = lax.broadcasted_iota(jnp.int32, (TILE, LANES), 0) < TILE // 2
    side = jnp.where(upper, F32(1.0), F32(-1.0))

    def tile(values, number):
        return values[number * TILE : (number + 1) * TILE]

    def spread(values, signed):
        turned = flipped(values)
        found = []
        for number in range(tiles):
            here, there = tile(values, number // 2), tile(turned, number // 2)
            if number % 2:
                here, there = there, here
            both = jnp.where(upper, here, there)
            found.append(both * side if signed else both)
        return found

    def part(found, chunk):
        return jnp.concatenate(found[chunk * count : (chunk + 1) * count], axis=0)

    def ones(values, bits):
        return sum((values >> bit) & 1 for bit in range(bits))

    small_row = lax.broadcasted_iota(jnp.int32, (TILE, LANES), 0)
    small_lane = lax.broadcasted_iota(jnp.int32, (TILE, LANES), 1)
    held_ones = ones(small_lane, LANE_BITS) + sum(
        lax.rem(lax.div(me, 2**bit), 2) for bit in range(global_bits)
    )
    quarters = [
        ((held_ones + ones(small_row, 3) + more) & 3).astype(F32) * F32(-math.pi / 2)
        for more in range(4)
    ]
    frame = jnp.concatenate(
        [quarters[number.bit_count() & 3] for number in range(rows // TILE)], axis=0
    )

    def doubled(first, step):
        found = [first]
        for bit in range(3, row_bits):
            found = sum(zip(*[step(value, bit) for value in found]), ())
        return jnp.concatenate(found, axis=0)

    def own_spin(bit):
        if bit < row_bits:
            return (1 - 2 * ((small_row >> bit) & 1)).astype(F32)
        bit = bit - row_bits
        return (1 - 2 * lax.rem(lax.div(me, 2**bit), 2)).astype(F32)

    own_bits = list(range(3)) + list(range(row_bits, row_bits + global_bits))
    above = small_lane - LANE_BITS
    first_spin = jnp.where((above >= 0) & (above < row_bits), F32(1.0), F32(0.0))
    for bit in own_bits:
        first_spin = jnp.where(above == bit, own_spin(bit), first_spin)
    bonds = couplings([0])[0]

    def bond_row(bit):
        return bonds[LANE_BITS + bit : LANE_BITS + bit + 1]

    spin = doubled(
        first_spin,
        lambda value, bit: (value, jnp.where(above == bit, -value, value)),
    )
    half = doubled(
        sum(own_spin(bit) * bond_row(bit) for bit in own_bits),
        lambda value, bit: (value + bond_row(bit), value - bond_row(bit)),
    )
    sine, cosine = sin_cos(field(spin, bonds, False, half) + frame)
    lanes = right_operand(rotation([turn(0, qubit) for qubit in range(LANE_BITS)], True))
    held = split(rotation([turn(0, LANE_BITS + bit) for bit in range(row_bits)]))

    arrivals[-1].wait()
    real = state_ref[pl.ds(0, rows, 2), :]
    imag = state_ref[pl.ds(1, rows, 2), :]
    norm_send[...] = jnp.sum(real * real + imag * imag, axis=0, keepdims=True)
    real, imag = cosine * real + sine * imag, cosine * imag - sine * real
    both = apply_lanes(jnp.concatenate([real, imag], axis=0), lanes)
    both = mm3(held, split(jnp.concatenate([both[:rows], both[rows:]], axis=1)))
    real, imag = both[:, :LANES], both[:, LANES:]
    turned_real, turned_imag = flipped(real), flipped(imag)
    norms, weights = stat_copies(0), stat_copies(1)
    def pack(unit):
        for chunk in range(unit * depth, unit * depth + depth):
            for block in range(count):
                number = block * chunks + chunk
                if number % 2:
                    ends = tile(turned_real, number // 2), tile(imag, number // 2)
                else:
                    ends = tile(real, number // 2), tile(turned_imag, number // 2)
                send[0, unit, block, shelf(chunk), :] = jnp.where(upper, *ends)

    pack(0)
    def launch(layer, unit):
        for place, plan in ((outer, PLANS[layer][unit % 2]), (inner, INNER[layer][unit % 2])):
            @pl.when(place)
            def _():
                for copy in copies(layer, unit, ranked(*plan)):
                    copy.start()

    def begin(groups):
        for group in groups:
            steps = [group * quarter + low for low in reversed(range(quarter))]
            for copy in copies(0, 0, [step for step in steps if step]):
                copy.start()

    pl.semaphore_wait(barrier, 2 * quarter - 1 + middle * quarter)

    @pl.when(inner)
    def _():
        greet(near_sem, 3 * quarter)
        greet(near_sem, quarter)
        begin((3,))

    begin((1, 0))
    for unit in range(1, units):
        pack(unit)
    pl.semaphore_wait(near_sem, 1)

    @pl.when(inner)
    def _():
        greet(far_sem, quarter)
        begin((2,))

    @pl.when(outer)
    def _():
        begin((2,))
        pl.semaphore_wait(far_sem, 1)
        begin((3,))

    for unit in range(units):
        recv[0, unit, me] = send[0, unit, me]
    norm_recv[me] = norm_send[...]

    moved = row_spin(True, True)
    next_bonds, sign_bonds = couplings([1, LAYERS])
    sine, cosine = sin_cos(field(moved, next_bonds, False))
    sine, cosine = spread(sine, True), spread(cosine, False)
    for unit in range(1, units):
        launch(0, unit)
    for copy in norms:
        copy.start()
    lanes = right_operand(rotation([turn(1, qubit) for qubit in range(LANE_BITS)], True))
    held = jnp.concatenate(
        split(
            rotation(
                [turn(1, LANE_BITS + bit) for bit in range(inner_bits)]
                + [None]
                + [turn(1, local_bits + bit) for bit in range(global_bits)]
            )
        ),
        axis=1,
    )
    late = [turn(1, LANE_BITS + inner_bits + bit) for bit in range(chunk_bits)]
    tops = [
        [turn(0, local_bits + bit) for bit in range(global_bits)],
        [turn(1, local_bits - global_bits + bit) for bit in range(global_bits)],
    ]
    energy_moved = spread(field(moved, sign_bonds, True), False)
    energy_plain = spread(field(row_spin(False, True), sign_bonds, True), False)

    def folded(parts, energy_field):
        total = jnp.zeros((TILE, LANES), F32)
        for chunk, values in enumerate(parts):
            weight = values * values * part(energy_field, chunk)
            for block in range(count):
                total = total + tile(weight, block)
        return jnp.sum(total, axis=0, keepdims=True)

    between = []
    for chunk in range(chunks):
        if chunk % depth == 0:
            blocks(0, chunk // depth).wait_recv()
        values = turn_blocks(received(0, chunk), tops[0])
        between.append(values)
        values = part(cosine, chunk) * values + part(sine, chunk) * flipped(values)
        values = apply_lanes(values, lanes)
        values = paired(held, right_operand(values))
        unit = chunk // depth
        send[1, unit, :, shelf(chunk), :] = values.reshape(count, TILE, LANES)
        if chunk % depth == depth - 1:
            launch(1, unit)
            recv[1, unit, me] = send[1, unit, me]

    energy_send[0:1] = folded(between, energy_moved)
    stats(0).wait_recv()
    amps_total = F32(2.0**qubits)
    norm = jnp.sum(jnp.sum(norm_recv[...], axis=0), axis=1, keepdims=True)
    factor = 1.0 / jnp.sqrt(norm / amps_total + 1e-06)
    phase = (held_ones + ones(small_row, inner_bits)) & 3
    even = (phase & 1) == 0
    sign = jnp.where((phase & 2) == 0, factor, -factor)
    along, across = jnp.where(even, sign, 0.0), jnp.where(even, 0.0, sign)
    frames = [
        (along, across * side),
        (-across, along * side),
        (-along, -across * side),
        (across, -along * side),
    ]

    parts = []
    for chunk in range(chunks):
        if chunk % depth == 0:
            blocks(1, chunk // depth).wait_recv()
        parts.append(turn_blocks(received(1, chunk), tops[1]))
        for bit, (cosine, sine) in enumerate(late):
            if (chunk + 1) % (2 << bit) == 0:
                for high in range(chunk + 1 - (1 << bit), chunk + 1):
                    low = high - (1 << bit)
                    parts[low], parts[high] = (
                        cosine * parts[low] - sine * parts[high],
                        cosine * parts[high] + sine * parts[low],
                    )

    energy_send[1:2] = folded(parts, energy_plain)
    for copy in weights:
        copy.start()
    energy_recv[me] = energy_send[...]
    for chunk, values in enumerate(parts):
        turned = flipped(values)
        for block in range(count):
            along, across = frames[(block.bit_count() + chunk.bit_count()) & 3]
            final = along * tile(values, block) + across * tile(turned, block)
            start = TILE * (block * chunks + chunk)
            out_ref[pl.ds(start, chunk_rows, 2), :] = final[:chunk_rows]
            out_ref[pl.ds(start + 1, chunk_rows, 2), :] = final[chunk_rows:]
    pltpu.make_async_remote_copy(
        src_ref=send.at[:, :, others],
        dst_ref=recv.at[:, :, others],
        send_sem=send_sem,
        recv_sem=recv_sems.at[0, 0],
        device_id={axis: peers[order[0]]},
        device_id_type=MESH,
    ).wait_send()
    stats(0).wait_send()
    stats(1).wait_recv()
    sums = jnp.sum(energy_recv[...], axis=0) * (factor * factor / amps_total)
    sums = jnp.sum(sums, axis=1, keepdims=True)
    which = lax.broadcasted_iota(jnp.int32, (1, LAYERS), 1)
    energy_ref[...] = jnp.where(which == 0, sums[0:1], sums[1:2])
    stats(1).wait_send()


def place(state_ref, energy_ref, state_out, energy_out, sems):
    moves = [
        pltpu.make_async_copy(state_ref, state_out, sems.at[0]),
        pltpu.make_async_copy(energy_ref, energy_out, sems.at[1]),
    ]
    for move in moves:
        move.start()
    for move in moves:
        move.wait()


def solution(mesh):
    axis = "amp"
    count = mesh.shape[axis]

    def local(amplitudes, coupling_index, rotation_index, chain_order, bond_sign):
        rows = amplitudes.shape[1] // LANES
        qubits = chain_order.shape[0]
        block_rows = rows // count
        chunk_rows = TILE // 2
        chunks = block_rows // chunk_rows
        depth = 2 if chunks % 2 == 0 else 1
        units = chunks // depth
        view = amplitudes.reshape(2, rows, LANES).transpose(1, 0, 2).reshape(2 * rows, LANES)
        vmem = pl.BlockSpec(memory_space=pltpu.VMEM)
        anywhere = pl.BlockSpec(memory_space=pl.ANY)
        state, energies = pl.pallas_call(
            functools.partial(kernel, axis, count, chunks, depth, qubits),
            out_shape=(
                pltpu.VMEM((2 * rows, LANES), F32),
                pltpu.VMEM((1, LAYERS), F32),
            ),
            in_specs=[anywhere] * 5,
            out_specs=(vmem, vmem),
            scratch_shapes=[
                pltpu.VMEM((2 * rows, LANES), F32),
                pltpu.SMEM(coupling_index.shape, jnp.int32),
                pltpu.SMEM(rotation_index.shape, jnp.int32),
                pltpu.SMEM(chain_order.shape, jnp.int32),
                pltpu.SMEM(bond_sign.shape, jnp.int32),
                pltpu.SMEM((2, ANGLES), F32),
                pltpu.VMEM((LAYERS, units, count, depth * TILE, LANES), F32),
                pltpu.VMEM((LAYERS, units, count, depth * TILE, LANES), F32),
                pltpu.VMEM((1, LANES), F32),
                pltpu.VMEM((count, 1, LANES), F32),
                pltpu.VMEM((LAYERS, LANES), F32),
                pltpu.VMEM((count, LAYERS, LANES), F32),
                pltpu.SemaphoreType.DMA((5,)),
                pltpu.SemaphoreType.DMA,
                pltpu.SemaphoreType.DMA((LAYERS, units)),
                pltpu.SemaphoreType.DMA((2,)),
                pltpu.SemaphoreType.DMA((2,)),
                pltpu.SemaphoreType.REGULAR,
                pltpu.SemaphoreType.REGULAR,
            ],
            compiler_params=pltpu.CompilerParams(collective_id=0, has_side_effects=True),
        )(view, coupling_index, rotation_index, chain_order, bond_sign)
        state, energies = pl.pallas_call(
            place,
            out_shape=(
                jax.ShapeDtypeStruct((2 * rows, LANES), F32),
                jax.ShapeDtypeStruct((1, LAYERS), F32),
            ),
            in_specs=[anywhere] * 2,
            out_specs=(anywhere, anywhere),
            scratch_shapes=[pltpu.SemaphoreType.DMA((2,))],
        )(*(pltpu.with_memory_space_constraint(x, pltpu.VMEM) for x in (state, energies)))
        state = state.reshape(rows, 2, LANES).transpose(1, 0, 2).reshape(2, rows * LANES)
        return state, energies.reshape(LAYERS)

    in_specs = (P(None, ("rep", "amp")), P("rep", None), P("rep", None), P(), P())
    out_specs = (P(None, ("rep", "amp")), P("rep"))
    return jax.shard_map(local, mesh=mesh, in_specs=in_specs, out_specs=out_specs, check_vma=False)
```
